256 devices in a mesh: row: 8 (over x, core), col: 32 (over z, y).
Axes of the slice: x: 4, y: 4, z: 8, core: 2. Of those that a mesh axis runs over, the one named last changes fastest.
Arguments:
- x_rows: float32 [16, 32768], P(None, ('row', 'col')), may hold values from -6 to 6
- alpha_rows: float32 [32768], P(('row', 'col')), may hold values from -0.5 to 1.5
- x_cols: float32 [16, 32768], P(None, ('col', 'row')), may hold values from -6 to 6
- alpha_cols: float32 [32768], P(('col', 'row')), may hold values from -0.0018310547 to 0.005493164
- lengthscale: float32 [16], replicated, may hold values from 1.2 to 2.5
Outputs:
- row_terms: float32 [16, 32768], P(None, ('row', 'col'))
- kernel_alpha: float32 [32768], P(('row', 'col'))
- grad: float32 [16], replicated
The draws below stay inside these ranges and needn't reach their ends.
All inputs are finite; a program needn't handle non-finite values.
Results may differ from the reference program's by a relative error of at most 0.00021.
Values sent between devices are 32-bit elements; how exact they have to be, the bound alone decides.
No kernel may reach another device: no remote copies, remote signals or barrier semaphores. Data moves between devices by JAX's collectives and lax.ppermute only.
A program may use at most 64 MiB of HBM per device.

```python
import math
import jax
import jax.numpy as jnp
from jax import lax

DIMS = 16
ROWS = 32768
NPTS = 32768


def block_levels(rng, shape, split, low, high):
    gain = 1.0
    for position, parts in split:
        draws = jax.random.uniform(jax.random.fold_in(jax.random.fold_in(rng, 6), position), (parts,), jnp.float32, low / len(split), high / len(split))
        gain = gain * jnp.repeat(jnp.exp(draws), shape[position] // parts).reshape((-1,) + (1,) * (len(shape) - 1 - position))
    return gain


def bell_draw(stream_key, extent, spread, most, shards=(), kind=jnp.bfloat16):
    entries = jax.random.normal(stream_key, extent, jnp.float32) * spread
    if len(shards) > 0:
        entries = block_levels(stream_key, extent, shards, -0.22, 0.18) * entries
    return jnp.clip(entries, min=-most, max=most).astype(kind)


def setup_inputs(seed: int = 0) -> dict:
    seeds = jax.random.split(jax.random.key(seed), 6)
    return {
        "x_rows": bell_draw(seeds[0], (DIMS, ROWS), 1.0, 6.0, ((1, 256),), jnp.float32),
        "alpha_rows": jnp.clip(-0.5 + 2.0 * jax.random.uniform(seeds[1], (ROWS,), jnp.float32) ** block_levels(seeds[1], (ROWS,), ((0, 256),), -0.2, 0.2), -0.5, 1.5),
        "x_cols": bell_draw(seeds[2], (DIMS, NPTS), 1.0, 6.0, ((1, 256),), jnp.float32),
        "alpha_cols": jnp.clip(-0.0018310547 + 0.0073242188 * jax.random.uniform(seeds[3], (NPTS,), jnp.float32) ** block_levels(seeds[3], (NPTS,), ((0, 256),), -0.2, 0.2), -0.0018310547, 0.005493164),
        "lengthscale": jnp.clip(jnp.exp(jax.random.uniform(seeds[4], (DIMS,), jnp.float32, math.log(1.2), math.log(2.5))), 1.2, 2.5),
    }


def fold_terms(partials, row_scaled, row_alpha):
    dims = row_scaled.shape[0]
    weight_sum = partials[0]
    first_moment = partials[1:1 + dims]
    second_moment = partials[1 + dims:]
    terms = 0.5 * row_alpha[None, :] * (row_scaled * row_scaled * weight_sum[None, :] - 2.0 * row_scaled * first_moment + second_moment)
    return terms, weight_sum


def reference(x_rows, alpha_rows, x_cols, alpha_cols, lengthscale):
    inverse_scale = 1.0 / lengthscale
    row_scaled = x_rows * inverse_scale[:, None]
    col_scaled = x_cols * inverse_scale[:, None]
    col_norms = jnp.sum(col_scaled * col_scaled, 0)
    values = jnp.concatenate([alpha_cols[None, :], alpha_cols[None, :] * col_scaled, alpha_cols[None, :] * col_scaled * col_scaled], 0)
    block_rows = min(512, ROWS)
    block_count = ROWS // block_rows
    blocks = jnp.transpose(row_scaled.reshape(DIMS, block_count, block_rows), (1, 0, 2))

    def one_block(row_block):
        row_norms = jnp.sum(row_block * row_block, 0)
        cross = lax.dot_general(row_block, col_scaled, (((0,), (0,)), ((), ())), precision=lax.Precision.HIGHEST, preferred_element_type=jnp.float32)
        kernel = jnp.exp(-0.5 * (row_norms[:, None] + col_norms[None, :] - 2.0 * cross))
        return lax.dot_general(values, kernel, (((1,), (1,)), ((), ())), precision=lax.Precision.HIGHEST, preferred_element_type=jnp.float32)

    pieces = lax.map(one_block, blocks)
    partials = jnp.transpose(pieces, (1, 0, 2)).reshape(2 * DIMS + 1, ROWS)
    terms, weight_sum = fold_terms(partials, row_scaled, alpha_rows)
    grad = jnp.sum(terms, 1) / ROWS
    return terms, weight_sum, grad
```

```python
import functools
import math

import jax
import jax.numpy as jnp
from jax import lax
from jax.experimental import pallas as pl
from jax.experimental.pallas import tpu as pltpu
from jax.sharding import Mesh
from jax.sharding import PartitionSpec as P

ROW = ("row_0", "row_1")
COL = ("col_0", "col_1")
ROW_COL = ("row_0", "row_1", "col_0", "col_1")
COL_ROW = ("col_0", "col_1", "row_0", "row_1")
LOG2E = math.log2(math.e)
LANES = 128
TILE = 256


def split3(x):
    high = x.astype(jnp.bfloat16).astype(jnp.float32)
    rest = x - high
    middle = rest.astype(jnp.bfloat16).astype(jnp.float32)
    return high, middle, rest - middle


def placed_rows(entries, height, lanes):
    row = lax.broadcasted_iota(jnp.int32, (height, lanes), 0)
    block = jnp.zeros((height, lanes), jnp.float32)
    for k, entry in enumerate(entries):
        block = jnp.where(row == k, entry, block)
    return block


def inverse_scales(scale_ref, dims):
    scales = jnp.broadcast_to(scale_ref[:, :dims], (dims, dims))
    row = lax.broadcasted_iota(jnp.int32, (dims, dims), 0)
    lane = lax.broadcasted_iota(jnp.int32, (dims, dims), 1)
    column = jnp.sum(jnp.where(row == lane, scales, 0.0), 1, keepdims=True)
    return 1.0 / column


def tile_kernel(rows_ref, cols_ref, scale_ref, out_ref, a_ref, b_ref, v_ref):
    row_chunks, entries, lanes = rows_ref.shape
    col_chunks = cols_ref.shape[0]
    dims = entries - 1
    bf16 = jnp.bfloat16
    inverse = inverse_scales(scale_ref, dims)
    root = math.sqrt(LOG2E)

    for p in range(row_chunks):
        scaled = rows_ref[p, :dims, :] * inverse * root
        norm = -0.5 * jnp.sum(scaled * scaled, 0, keepdims=True)
        h, m, l = split3(scaled)
        nh, nm, nl = split3(norm)
        norms = placed_rows((nh, nm, nl, 1.0, 1.0, 1.0), dims, lanes)
        blocks = (h, h, m, m, h, l, norms, jnp.zeros_like(norms))
        for g, block in enumerate(blocks):
            a_ref[g * dims:(g + 1) * dims, p * lanes:(p + 1) * lanes] = block.astype(bf16)

    def prepare(p, carry):
        unit = cols_ref[p, :dims, :] * inverse
        alpha = cols_ref[p, dims:dims + 1, :]
        scaled = unit * root
        norm = -0.5 * jnp.sum(scaled * scaled, 0, keepdims=True)
        h, m, l = split3(scaled)
        nh, nm, nl = split3(norm)
        norms = placed_rows((1.0, 1.0, 1.0, nh, nm, nl), dims, lanes)
        stacked = jnp.concatenate([h, m, h, m, l, h, norms, jnp.zeros_like(norms)], 0)
        start = pl.multiple_of(p * lanes, lanes)
        b_ref[pl.ds(start, lanes), :] = stacked.T.astype(bf16)
        fh, fm, fl = split3(alpha * unit)
        sh, sm, sl = split3(alpha * unit * unit)
        alphas = placed_rows(split3(alpha), dims, lanes)
        for g, block in enumerate((fh, fm, sh, sm, alphas, fl, sl)):
            v_ref[g * dims:(g + 1) * dims, pl.ds(start, lanes)] = block.astype(bf16)
        return carry

    lax.fori_loop(0, col_chunks, prepare, 0, unroll=4)

    col_count = col_chunks * lanes
    grad = jnp.zeros((dims, lanes), jnp.float32)
    for t in range(row_chunks * lanes // TILE):
        a_tile = a_ref[:, t * TILE:(t + 1) * TILE]

        def step(c, total):
            start = pl.multiple_of(c * STEP, STEP)
            exponent = jnp.dot(b_ref[pl.ds(start, STEP), :], a_tile, preferred_element_type=jnp.float32)
            kernel = jnp.exp2(exponent)
            high = kernel.astype(bf16)
            low = (kernel - high.astype(jnp.float32)).astype(bf16)
            from_high = jnp.dot(v_ref[:, pl.ds(start, STEP)], high, preferred_element_type=jnp.float32)
            from_low = jnp.dot(v_ref[:5 * dims, pl.ds(start, STEP)], low, preferred_element_type=jnp.float32)
            return total[0] + from_high, total[1] + from_low

        zeros = (jnp.zeros((7 * dims, TILE), jnp.float32), jnp.zeros((5 * dims, TILE), jnp.float32))
        big, small = lax.fori_loop(0, col_count // STEP, step, zeros, unroll=UNROLL)
        part = lambda x, g: x[g * dims:(g + 1) * dims]
        first = (part(small, 0) + part(small, 1) + part(big, 5)) + part(big, 1) + part(big, 0)
        second = (part(small, 2) + part(small, 3) + part(big, 6)) + part(big, 3) + part(big, 2)
        weights = part(big, 4) + part(small, 4)
        weight = weights[0:1] + weights[1:2] + weights[2:3]
        for q in range(TILE // lanes):
            p = t * (TILE // lanes) + q
            cut = slice(q * lanes, (q + 1) * lanes)
            scaled = rows_ref[p, :dims, :] * inverse
            row_alpha = rows_ref[p, dims:dims + 1, :]
            terms = 0.5 * row_alpha * (scaled * scaled * weight[:, cut] - 2.0 * scaled * first[:, cut] + second[:, cut])
            out_ref[p, :dims, :] = terms
            out_ref[p, dims:dims + 1, :] = weight[:, cut]
            grad = grad + terms
    column = jnp.sum(grad, 1, keepdims=True)
    row = lax.broadcasted_iota(jnp.int32, (dims, lanes), 0)
    lane = lax.broadcasted_iota(jnp.int32, (dims, lanes), 1)
    shares = jnp.sum(jnp.where(row == lane, column, 0.0), 0, keepdims=True)
    for p in range(row_chunks):
        out_ref[p, dims + 1:dims + 2, :] = shares


STEP = 512
UNROLL = 2


def tile_terms(rows, cols, lengthscale):
    row_chunks, entries, lanes = rows.shape
    col_chunks = cols.shape[0]
    dims = entries - 1
    whole = pl.BlockSpec(memory_space=pltpu.VMEM)
    pairs = row_chunks * col_chunks * lanes * lanes
    return pl.pallas_call(
        tile_kernel,
        out_shape=jax.ShapeDtypeStruct((row_chunks, entries + 1, lanes), jnp.float32),
        in_specs=[whole, whole, whole],
        out_specs=whole,
        scratch_shapes=[
            pltpu.VMEM((8 * dims, row_chunks * lanes), jnp.bfloat16),
            pltpu.VMEM((col_chunks * lanes, 8 * dims), jnp.bfloat16),
            pltpu.VMEM((7 * dims, col_chunks * lanes), jnp.bfloat16),
        ],
        cost_estimate=pl.CostEstimate(flops=600 * pairs, bytes_accessed=1 << 20, transcendentals=pairs),
        name="tile_terms",
    )(rows, cols, lengthscale.reshape(1, dims))


def copies(x, axes):
    blocks = jnp.broadcast_to(x, (lax.axis_size(axes), *x.shape))
    return lax.all_to_all(blocks, axes, split_axis=0, concat_axis=0, tiled=True)


def on_device(x_rows, alpha_rows, x_cols, alpha_cols, lengthscale):
    dims = x_rows.shape[0]
    rows = copies(jnp.concatenate([x_rows, alpha_rows[None, :]], 0), ROW)
    cols = copies(jnp.concatenate([x_cols, alpha_cols[None, :]], 0), COL)
    parts = tile_terms(rows, cols, lengthscale)
    arrived = lax.all_to_all(parts, ROW, split_axis=0, concat_axis=0, tiled=True)
    summed = arrived.sum(axis=0)
    shares = copies(summed[dims + 1:], COL)
    total_rows = x_rows.shape[1] * lax.axis_size(ROW_COL)
    grad = shares.sum(axis=(0, 1))[:dims] / total_rows
    return summed[:dims], summed[dims], grad


def solution(mesh):
    finer = Mesh(mesh.devices.reshape(4, 2, 8, 4), ROW_COL)
    in_specs = (P(None, ROW_COL), P(ROW_COL), P(None, COL_ROW), P(COL_ROW), P())
    out_specs = (P(None, ROW_COL), P(ROW_COL), P())
    return jax.shard_map(on_device, mesh=finer, in_specs=in_specs, out_specs=out_specs, check_vma=False)
```

```python
import math

import jax
import jax.numpy as jnp
from jax import lax
from jax.experimental import pallas as pl
from jax.experimental.pallas import tpu as pltpu
from jax.sharding import Mesh
from jax.sharding import PartitionSpec as P

ROW_COL = ("row_0", "row_1", "col_0", "col_1")
COL_ROW = ("col_0", "col_1", "row_0", "row_1")
LOG2E = math.log2(math.e)
LANES = 128
COL_CLASSES = 8
STEP = 512
UNROLL = 2


def split3(x):
    high = x.astype(jnp.bfloat16).astype(jnp.float32)
    rest = x - high
    middle = rest.astype(jnp.bfloat16).astype(jnp.float32)
    return high, middle, rest - middle


def placed_rows(entries, height, lanes):
    row = lax.broadcasted_iota(jnp.int32, (height, lanes), 0)
    block = jnp.zeros((height, lanes), jnp.float32)
    for k, entry in enumerate(entries):
        block = jnp.where(row == k, entry, block)
    return block


def to_left(x, lanes):
    return pltpu.roll(x, (LANES - lanes) % LANES, 1)


def to_right(x, lanes):
    return pltpu.roll(x, lanes % LANES, 1)


class Plan:
    def __init__(self, devices, dims, points):
        self.devices, self.dims = devices, dims
        self.cols = COL_CLASSES
        self.rows = devices // self.cols
        self.row_each = points // self.rows
        self.col_each = points // self.cols
        self.at_cols = self.row_each * dims
        self.at_col_alpha = self.at_cols + self.col_each * dims
        self.at_row_alpha = self.at_col_alpha + self.col_each
        self.tiles = pl.cdiv(self.at_row_alpha + self.row_each, LANES)
        self.at_weight = self.row_each * dims
        self.at_grad = self.at_weight + pl.cdiv(self.row_each, 8) * 8


def spread_kernel(plan, rows_ref, row_alpha_ref, cols_ref, col_alpha_ref, scale_ref, out_ref):
    dims = plan.dims
    scales = jnp.broadcast_to(scale_ref[:, :dims], (dims, dims))
    down = lax.broadcasted_iota(jnp.int32, (dims, dims), 0)
    along = lax.broadcasted_iota(jnp.int32, (dims, dims), 1)
    inverse = 1.0 / jnp.sum(jnp.where(down == along, scales, 0.0), 1, keepdims=True)
    rows = rows_ref[...] * inverse
    cols = cols_ref[...] * inverse
    pieces = [to_left(rows, i * plan.rows) for i in range(plan.row_each)]
    pieces += [to_left(cols, i * plan.cols) for i in range(plan.col_each)]
    alphas = [to_left(col_alpha_ref[...], i * plan.cols) for i in range(plan.col_each)]
    alphas += [to_left(row_alpha_ref[...], i * plan.rows) for i in range(plan.row_each)]
    left = plan.tiles * LANES - plan.at_col_alpha
    pieces.append(placed_rows(alphas, left, LANES))
    stacked = jnp.concatenate(pieces, 0)
    for k in range(plan.tiles):
        turned = stacked[k * LANES:(k + 1) * LANES].T
        lane = lax.broadcasted_iota(jnp.int32, (plan.cols, LANES), 1) + k * LANES
        is_row = (lane < plan.at_cols) | (lane >= plan.at_row_alpha)
        of_cols = turned[:plan.cols]
        for r in range(plan.rows):
            of_row = jnp.broadcast_to(turned[r:r + 1], (plan.cols, LANES))
            start = r * plan.cols * plan.tiles + k
            out_ref[pl.ds(start, plan.cols, stride=plan.tiles), :] = jnp.where(is_row, of_row, of_cols)


def tile_kernel(plan, in_ref, out_ref, t_ref, a_ref, b_ref, v_ref, o_ref):
    dims, width = plan.dims, plan.devices
    bf16 = jnp.bfloat16
    root = math.sqrt(LOG2E)
    for k in range(plan.tiles):
        t_ref[k * LANES:(k + 1) * LANES, :] = in_ref[pl.ds(k, width, stride=plan.tiles), :].T

    def exponents(unit, ones_first):
        scaled = unit * root
        norm = -0.5 * jnp.sum(scaled * scaled, 0, keepdims=True)
        parts = split3(norm)
        ones = (1.0, 1.0, 1.0)
        norms = placed_rows(ones + parts if ones_first else parts + ones, dims, width)
        return *split3(scaled), norms

    for i in range(plan.row_each):
        h, m, l, norms = exponents(t_ref[i * dims:(i + 1) * dims, :], False)
        blocks = (h, h, m, m, h, l, norms, jnp.zeros_like(norms))
        for g, block in enumerate(blocks):
            a_ref[g * dims:(g + 1) * dims, i * width:(i + 1) * width] = block.astype(bf16)

    for i in range(plan.col_each):
        at = plan.at_cols + i * dims
        unit = t_ref[at:at + dims, :]
        alpha = t_ref[plan.at_col_alpha + i:plan.at_col_alpha + i + 1, :]
        h, m, l, norms = exponents(unit, True)
        stacked = jnp.concatenate([h, m, h, m, l, h, norms, jnp.zeros_like(norms)], 0)
        b_ref[i * width:(i + 1) * width, :] = stacked.astype(bf16).T
        weighted = alpha * unit
        fh, fm, fl = split3(weighted)
        sh, sm, sl = split3(weighted * unit)
        alphas = placed_rows(split3(alpha), dims, width)
        for g, block in enumerate((fh, fm, sh, sm, alphas, fl, sl)):
            v_ref[g * dims:(g + 1) * dims, i * width:(i + 1) * width] = block.astype(bf16)

    col_count = plan.col_each * width
    grad = jnp.zeros((dims, width), jnp.float32)
    o_ref[plan.at_weight:, :] = jnp.zeros((LANES - plan.at_weight, width), jnp.float32)
    for i in range(plan.row_each):
        a_tile = a_ref[:, i * width:(i + 1) * width]

        def step(c, total):
            start = pl.multiple_of(c * STEP, STEP)
            exponent = jnp.dot(b_ref[pl.ds(start, STEP), :], a_tile, preferred_element_type=jnp.float32)
            kernel = jnp.exp2(exponent)
            high = kernel.astype(bf16)
            low = (kernel - high.astype(jnp.float32)).astype(bf16)
            from_high = jnp.dot(v_ref[:, pl.ds(start, STEP)], high, preferred_element_type=jnp.float32)
            from_low = jnp.dot(v_ref[:5 * dims, pl.ds(start, STEP)], low, preferred_element_type=jnp.float32)
            return total[0] + from_high, total[1] + from_low

        zeros = (jnp.zeros((7 * dims, width), jnp.float32), jnp.zeros((5 * dims, width), jnp.float32))
        big, small = lax.fori_loop(0, col_count // STEP, step, zeros, unroll=UNROLL)

        def part(x, g):
            return x[g * dims:(g + 1) * dims]

        first = (part(small, 0) + part(small, 1) + part(big, 5)) + part(big, 1) + part(big, 0)
        second = (part(small, 2) + part(small, 3) + part(big, 6)) + part(big, 3) + part(big, 2)
        weights = part(big, 4) + part(small, 4)
        weight = weights[0:1] + weights[1:2] + weights[2:3]
        unit = t_ref[i * dims:(i + 1) * dims, :]
        alpha = t_ref[plan.at_row_alpha + i:plan.at_row_alpha + i + 1, :]
        terms = 0.5 * alpha * (unit * unit * weight - 2.0 * unit * first + second)
        o_ref[i * dims:(i + 1) * dims, :] = terms
        o_ref[plan.at_weight + i:plan.at_weight + i + 1, :] = weight
        grad = grad + terms
    share = jnp.sum(grad, 1, keepdims=True)
    o_ref[plan.at_grad:plan.at_grad + dims, :] = jnp.broadcast_to(share, (dims, width))
    out_ref[...] = o_ref[...].T


def finish_kernel(plan, total_rows, in_ref, terms_ref, weight_ref, grad_ref):
    dims = plan.dims
    summed = jnp.sum(in_ref[...].reshape(plan.rows, plan.cols, LANES), 1)
    total = jnp.sum(summed, 0, keepdims=True)
    padded = jnp.concatenate([summed, jnp.zeros((LANES - plan.rows, LANES), jnp.float32)], 0)
    turned = padded.T
    terms = turned[:dims]
    weight = turned[plan.at_weight:plan.at_weight + 1]
    for i in range(1, plan.row_each):
        terms = terms + to_right(turned[i * dims:(i + 1) * dims], i * plan.rows)
        weight = weight + to_right(turned[plan.at_weight + i:plan.at_weight + i + 1], i * plan.rows)
    terms_ref[...] = terms
    weight_ref[...] = weight
    grad_ref[...] = to_left(total, plan.at_grad)[:, :dims] / total_rows


def on_device(x_rows, alpha_rows, x_cols, alpha_cols, lengthscale):
    dims, points = x_rows.shape
    devices = lax.axis_size(ROW_COL)
    plan = Plan(devices, dims, points)
    whole = pl.BlockSpec(memory_space=pltpu.VMEM)
    f32, bf16 = jnp.float32, jnp.bfloat16

    def exchanged(x, tiles):
        blocks = x.reshape(devices, 1, tiles * LANES)
        arrived = lax.all_to_all(blocks, ROW_COL, split_axis=0, concat_axis=0, tiled=True)
        return arrived.reshape(devices * tiles, LANES)

    blocks = pl.pallas_call(
        lambda *refs: spread_kernel(plan, *refs),
        out_shape=jax.ShapeDtypeStruct((devices * plan.tiles, LANES), f32),
        in_specs=[whole] * 5,
        out_specs=whole,
        name="spread",
    )(x_rows, alpha_rows.reshape(1, points), x_cols, alpha_cols.reshape(1, points), lengthscale.reshape(1, dims))
    gathered = exchanged(blocks, plan.tiles)
    row_count, col_count = plan.row_each * devices, plan.col_each * devices
    shares = pl.pallas_call(
        lambda *refs: tile_kernel(plan, *refs),
        out_shape=jax.ShapeDtypeStruct((devices, LANES), f32),
        in_specs=[whole],
        out_specs=whole,
        scratch_shapes=[
            pltpu.VMEM((plan.tiles * LANES, devices), f32),
            pltpu.VMEM((8 * dims, row_count), bf16),
            pltpu.VMEM((col_count, 8 * dims), bf16),
            pltpu.VMEM((7 * dims, col_count), bf16),
            pltpu.VMEM((LANES, devices), f32),
        ],
        name="tile",
    )(gathered)
    arrived = exchanged(shares, 1)
    terms, weight, grad = pl.pallas_call(
        lambda *refs: finish_kernel(plan, points * devices, *refs),
        out_shape=(
            jax.ShapeDtypeStruct((dims, points), f32),
            jax.ShapeDtypeStruct((1, points), f32),
            jax.ShapeDtypeStruct((1, dims), f32),
        ),
        in_specs=[whole],
        out_specs=(whole, whole, whole),
        name="finish",
    )(arrived)
    return terms, weight.reshape(points), grad.reshape(dims)


def solution(mesh):
    finer = Mesh(mesh.devices.reshape(4, 2, 8, 4), ROW_COL)
    in_specs = (P(None, ROW_COL), P(ROW_COL), P(None, COL_ROW), P(COL_ROW), P())
    out_specs = (P(None, ROW_COL), P(ROW_COL), P())
    return jax.shard_map(on_device, mesh=finer, in_specs=in_specs, out_specs=out_specs, check_vma=False)
```

```python
import math

import jax
import jax.numpy as jnp
from jax import lax
from jax.experimental import pallas as pl
from jax.experimental.pallas import tpu as pltpu
from jax.sharding import Mesh
from jax.sharding import PartitionSpec as P

ROW_COL = ("row_0", "row_1", "col_0", "col_1")
COL_ROW = ("col_0", "col_1", "row_0", "row_1")
LOG2E = math.log2(math.e)
LANES = 128
COL_CLASSES = 8
STEP = 512
UNROLL = 8


def split3(x):
    high = x.astype(jnp.bfloat16).astype(jnp.float32)
    rest = x - high
    middle = rest.astype(jnp.bfloat16).astype(jnp.float32)
    return high, middle, rest - middle


def placed_rows(entries, height, lanes):
    row = lax.broadcasted_iota(jnp.int32, (height, lanes), 0)
    block = jnp.zeros((height, lanes), jnp.float32)
    for k, entry in enumerate(entries):
        block = jnp.where(row == k, entry, block)
    return block


def to_left(x, lanes):
    return pltpu.roll(x, (LANES - lanes) % LANES, 1)


def to_right(x, lanes):
    return pltpu.roll(x, lanes % LANES, 1)


class Plan:
    def __init__(self, devices, dims, points):
        self.devices, self.dims = devices, dims
        self.cols = COL_CLASSES
        self.rows = devices // self.cols
        self.row_each = points // self.rows
        self.col_each = points // self.cols
        self.at_cols = self.row_each * dims
        self.at_col_alpha = self.at_cols + self.col_each * dims
        self.at_row_alpha = self.at_col_alpha + self.col_each
        self.tiles = pl.cdiv(self.at_row_alpha + self.row_each, LANES)
        self.at_weight = self.row_each * dims
        self.at_grad = self.at_weight + pl.cdiv(self.row_each, 8) * 8


def spread_kernel(plan, rows_ref, row_alpha_ref, cols_ref, col_alpha_ref, scale_ref, out_ref):
    dims = plan.dims
    scales = jnp.broadcast_to(scale_ref[:, :dims], (dims, dims))
    down = lax.broadcasted_iota(jnp.int32, (dims, dims), 0)
    along = lax.broadcasted_iota(jnp.int32, (dims, dims), 1)
    inverse = 1.0 / jnp.sum(jnp.where(down == along, scales, 0.0), 1, keepdims=True)
    rows = rows_ref[...] * inverse
    cols = cols_ref[...] * inverse
    pieces = [to_left(rows, i * plan.rows) for i in range(plan.row_each)]
    pieces += [to_left(cols, i * plan.cols) for i in range(plan.col_each)]
    alphas = [to_left(col_alpha_ref[...], i * plan.cols) for i in range(plan.col_each)]
    alphas += [to_left(row_alpha_ref[...], i * plan.rows) for i in range(plan.row_each)]
    left = plan.tiles * LANES - plan.at_col_alpha
    pieces.append(placed_rows(alphas, left, LANES))
    stacked = jnp.concatenate(pieces, 0)
    for k in range(plan.tiles):
        turned = stacked[k * LANES:(k + 1) * LANES].T
        lane = lax.broadcasted_iota(jnp.int32, (plan.cols, LANES), 1) + k * LANES
        is_row = (lane < plan.at_cols) | (lane >= plan.at_row_alpha)
        of_cols = turned[:plan.cols]
        for r in range(plan.rows):
            of_row = jnp.broadcast_to(turned[r:r + 1], (plan.cols, LANES))
            start = r * plan.cols * plan.tiles + k
            out_ref[pl.ds(start, plan.cols, stride=plan.tiles), :] = jnp.where(is_row, of_row, of_cols)


def tile_kernel(plan, in_ref, out_ref, t_ref, a_ref, b_ref, v_ref, o_ref):
    dims, width = plan.dims, plan.devices
    bf16 = jnp.bfloat16
    root = math.sqrt(LOG2E)
    for k in range(plan.tiles):
        t_ref[k * LANES:(k + 1) * LANES, :] = in_ref[pl.ds(k, width, stride=plan.tiles), :].T

    def exponents(unit, ones_first):
        scaled = unit * root
        norm = -0.5 * jnp.sum(scaled * scaled, 0, keepdims=True)
        parts = split3(norm)
        ones = (1.0, 1.0, 1.0)
        norms = placed_rows(ones + parts if ones_first else parts + ones, dims, width)
        return *split3(scaled), norms

    for i in range(plan.row_each):
        h, m, l, norms = exponents(t_ref[i * dims:(i + 1) * dims, :], False)
        blocks = (h, h, m, m, h, l, norms, jnp.zeros_like(norms))
        for g, block in enumerate(blocks):
            a_ref[g * dims:(g + 1) * dims, i * width:(i + 1) * width] = block.astype(bf16)

    for i in range(plan.col_each):
        at = plan.at_cols + i * dims
        unit = t_ref[at:at + dims, :]
        alpha = t_ref[plan.at_col_alpha + i:plan.at_col_alpha + i + 1, :]
        h, m, l, norms = exponents(unit, True)
        stacked = jnp.concatenate([h, m, h, m, l, h, norms, jnp.zeros_like(norms)], 0)
        b_ref[i * width:(i + 1) * width, :] = stacked.astype(bf16).T
        weighted = alpha * unit
        fh, fm, fl = split3(weighted)
        sh, sm, sl = split3(weighted * unit)
        alphas = placed_rows(split3(alpha), dims, width)
        for g, block in enumerate((fh, fm, sh, sm, alphas, fl, sl)):
            v_ref[g * dims:(g + 1) * dims, i * width:(i + 1) * width] = block.astype(bf16)

    col_count = plan.col_each * width
    grad = jnp.zeros((dims, width), jnp.float32)
    o_ref[plan.at_weight:, :] = jnp.zeros((LANES - plan.at_weight, width), jnp.float32)
    for i in range(plan.row_each):
        a_tile = a_ref[:, i * width:(i + 1) * width]

        def step(c, total):
            start = pl.multiple_of(c * STEP, STEP)
            exponent = jnp.dot(b_ref[pl.ds(start, STEP), :], a_tile, preferred_element_type=jnp.float32)
            kernel = jnp.exp2(exponent)
            high = kernel.astype(bf16)
            low = (kernel - high.astype(jnp.float32)).astype(bf16)
            from_high = jnp.dot(v_ref[:, pl.ds(start, STEP)], high, preferred_element_type=jnp.float32)
            from_low = jnp.dot(v_ref[:5 * dims, pl.ds(start, STEP)], low, preferred_element_type=jnp.float32)
            return total[0] + from_high, total[1] + from_low

        zeros = (jnp.zeros((7 * dims, width), jnp.float32), jnp.zeros((5 * dims, width), jnp.float32))
        big, small = lax.fori_loop(0, col_count // STEP, step, zeros, unroll=UNROLL)

        def part(x, g):
            return x[g * dims:(g + 1) * dims]

        first = (part(small, 0) + part(small, 1) + part(big, 5)) + part(big, 1) + part(big, 0)
        second = (part(small, 2) + part(small, 3) + part(big, 6)) + part(big, 3) + part(big, 2)
        weights = part(big, 4) + part(small, 4)
        weight = weights[0:1] + weights[1:2] + weights[2:3]
        unit = t_ref[i * dims:(i + 1) * dims, :]
        alpha = t_ref[plan.at_row_alpha + i:plan.at_row_alpha + i + 1, :]
        terms = 0.5 * alpha * (unit * unit * weight - 2.0 * unit * first + second)
        o_ref[i * dims:(i + 1) * dims, :] = terms
        o_ref[plan.at_weight + i:plan.at_weight + i + 1, :] = weight
        grad = grad + terms
    share = jnp.sum(grad, 1, keepdims=True)
    o_ref[plan.at_grad:plan.at_grad + dims, :] = jnp.broadcast_to(share, (dims, width))
    out_ref[...] = o_ref[...].T


def finish_kernel(plan, total_rows, in_ref, terms_ref, weight_ref, grad_ref):
    dims = plan.dims
    summed = jnp.sum(in_ref[...].reshape(plan.rows, plan.cols, LANES), 1)
    total = jnp.sum(summed, 0, keepdims=True)
    padded = jnp.concatenate([summed, jnp.zeros((LANES - plan.rows, LANES), jnp.float32)], 0)
    turned = padded.T
    terms = turned[:dims]
    weight = turned[plan.at_weight:plan.at_weight + 1]
    for i in range(1, plan.row_each):
        terms = terms + to_right(turned[i * dims:(i + 1) * dims], i * plan.rows)
        weight = weight + to_right(turned[plan.at_weight + i:plan.at_weight + i + 1], i * plan.rows)
    terms_ref[...] = terms
    weight_ref[...] = weight
    grad_ref[...] = to_left(total, plan.at_grad)[:, :dims] / total_rows


def on_device(x_rows, alpha_rows, x_cols, alpha_cols, lengthscale):
    dims, points = x_rows.shape
    devices = lax.axis_size(ROW_COL)
    plan = Plan(devices, dims, points)
    whole = pl.BlockSpec(memory_space=pltpu.VMEM)
    f32, bf16 = jnp.float32, jnp.bfloat16

    def exchanged(x, tiles):
        blocks = x.reshape(devices, 1, tiles * LANES)
        arrived = lax.all_to_all(blocks, ROW_COL, split_axis=0, concat_axis=0, tiled=True)
        return arrived.reshape(devices * tiles, LANES)

    blocks = pl.pallas_call(
        lambda *refs: spread_kernel(plan, *refs),
        out_shape=jax.ShapeDtypeStruct((devices * plan.tiles, LANES), f32),
        in_specs=[whole] * 5,
        out_specs=whole,
        name="spread",
    )(x_rows, alpha_rows.reshape(1, points), x_cols, alpha_cols.reshape(1, points), lengthscale.reshape(1, dims))
    gathered = exchanged(blocks, plan.tiles)
    row_count, col_count = plan.row_each * devices, plan.col_each * devices
    shares = pl.pallas_call(
        lambda *refs: tile_kernel(plan, *refs),
        out_shape=jax.ShapeDtypeStruct((devices, LANES), f32),
        in_specs=[whole],
        out_specs=whole,
        scratch_shapes=[
            pltpu.VMEM((plan.tiles * LANES, devices), f32),
            pltpu.VMEM((8 * dims, row_count), bf16),
            pltpu.VMEM((col_count, 8 * dims), bf16),
            pltpu.VMEM((7 * dims, col_count), bf16),
            pltpu.VMEM((LANES, devices), f32),
        ],
        name="tile",
    )(gathered)
    arrived = exchanged(shares, 1)
    terms, weight, grad = pl.pallas_call(
        lambda *refs: finish_kernel(plan, points * devices, *refs),
        out_shape=(
            jax.ShapeDtypeStruct((dims, points), f32),
            jax.ShapeDtypeStruct((1, points), f32),
            jax.ShapeDtypeStruct((1, dims), f32),
        ),
        in_specs=[whole],
        out_specs=(whole, whole, whole),
        name="finish",
    )(arrived)
    return terms, weight.reshape(points), grad.reshape(dims)


def solution(mesh):
    finer = Mesh(mesh.devices.reshape(4, 2, 8, 4), ROW_COL)
    in_specs = (P(None, ROW_COL), P(ROW_COL), P(None, COL_ROW), P(COL_ROW), P())
    out_specs = (P(None, ROW_COL), P(ROW_COL), P())
    return jax.shard_map(on_device, mesh=finer, in_specs=in_specs, out_specs=out_specs, check_vma=False)
```

```python
import math

import jax
import jax.numpy as jnp
from jax import lax
from jax.experimental import pallas as pl
from jax.experimental.pallas import tpu as pltpu
from jax.sharding import Mesh
from jax.sharding import PartitionSpec as P

ROW_COL = ("row_0", "row_1", "col_0", "col_1")
COL_ROW = ("col_0", "col_1", "row_0", "row_1")
LOG2E = math.log2(math.e)
LANES = 128
COL_CLASSES = 8
STEP = 512
UNROLL = 8


def split3(x):
    high = x.astype(jnp.bfloat16).astype(jnp.float32)
    rest = x - high
    middle = rest.astype(jnp.bfloat16).astype(jnp.float32)
    return high, middle, rest - middle


def placed_rows(entries, height, lanes):
    row = lax.broadcasted_iota(jnp.int32, (height, lanes), 0)
    block = jnp.zeros((height, lanes), jnp.float32)
    for k, entry in enumerate(entries):
        block = jnp.where(row == k, entry, block)
    return block


def to_left(x, lanes):
    return pltpu.roll(x, (LANES - lanes) % LANES, 1)


def to_right(x, lanes):
    return pltpu.roll(x, lanes % LANES, 1)


class Plan:
    def __init__(self, devices, dims, points):
        self.devices, self.dims = devices, dims
        self.cols = COL_CLASSES
        self.rows = devices // self.cols
        self.row_each = points // self.rows
        self.col_each = points // self.cols
        self.at_cols = self.row_each * dims
        self.at_col_alpha = self.at_cols + self.col_each * dims
        self.at_row_alpha = self.at_col_alpha + self.col_each
        self.tiles = pl.cdiv(self.at_row_alpha + self.row_each, LANES)
        self.at_weight = self.row_each * dims
        self.at_grad = self.at_weight + pl.cdiv(self.row_each, 8) * 8


def spread_kernel(plan, rows_ref, row_alpha_ref, cols_ref, col_alpha_ref, scale_ref, out_ref):
    dims = plan.dims
    scales = jnp.broadcast_to(scale_ref[:, :dims], (dims, dims))
    down = lax.broadcasted_iota(jnp.int32, (dims, dims), 0)
    along = lax.broadcasted_iota(jnp.int32, (dims, dims), 1)
    inverse = 1.0 / jnp.sum(jnp.where(down == along, scales, 0.0), 1, keepdims=True)
    rows = rows_ref[...] * inverse
    cols = cols_ref[...] * inverse
    pieces = [to_left(rows, i * plan.rows) for i in range(plan.row_each)]
    pieces += [to_left(cols, i * plan.cols) for i in range(plan.col_each)]
    alphas = [to_left(col_alpha_ref[...], i * plan.cols) for i in range(plan.col_each)]
    alphas += [to_left(row_alpha_ref[...], i * plan.rows) for i in range(plan.row_each)]
    left = plan.tiles * LANES - plan.at_col_alpha
    pieces.append(placed_rows(alphas, left, LANES))
    stacked = jnp.concatenate(pieces, 0)
    for k in range(plan.tiles):
        turned = stacked[k * LANES:(k + 1) * LANES].T
        lane = lax.broadcasted_iota(jnp.int32, (plan.cols, LANES), 1) + k * LANES
        is_row = (lane < plan.at_cols) | (lane >= plan.at_row_alpha)
        of_cols = turned[:plan.cols]
        for r in range(plan.rows):
            of_row = jnp.broadcast_to(turned[r:r + 1], (plan.cols, LANES))
            start = r * plan.cols * plan.tiles + k
            out_ref[pl.ds(start, plan.cols, stride=plan.tiles), :] = jnp.where(is_row, of_row, of_cols)


def tile_kernel(plan, in_ref, out_ref, t_ref, a_ref, b_ref, v_ref, o_ref):
    dims, width = plan.dims, plan.devices
    bf16 = jnp.bfloat16
    root = math.sqrt(LOG2E)
    for k in range(plan.tiles):
        t_ref[k * LANES:(k + 1) * LANES, :] = in_ref[pl.ds(k, width, stride=plan.tiles), :].T

    def exponents(unit, ones_first):
        scaled = unit * root
        norm = -0.5 * jnp.sum(scaled * scaled, 0, keepdims=True)
        parts = split3(norm)
        ones = (1.0, 1.0, 1.0)
        norms = placed_rows(ones + parts if ones_first else parts + ones, dims, width)
        return *split3(scaled), norms

    for i in range(plan.row_each):
        h, m, l, norms = exponents(t_ref[i * dims:(i + 1) * dims, :], False)
        blocks = (h, h, m, m, h, l, norms, jnp.zeros_like(norms))
        for g, block in enumerate(blocks):
            a_ref[g * dims:(g + 1) * dims, i * width:(i + 1) * width] = block.astype(bf16)

    for i in range(plan.col_each):
        at = plan.at_cols + i * dims
        unit = t_ref[at:at + dims, :]
        alpha = t_ref[plan.at_col_alpha + i:plan.at_col_alpha + i + 1, :]
        h, m, l, norms = exponents(unit, True)
        stacked = jnp.concatenate([h, m, h, m, l, h, norms, jnp.zeros_like(norms)], 0)
        b_ref[i * width:(i + 1) * width, :] = stacked.astype(bf16).T
        weighted = alpha * unit
        fh, fm, fl = split3(weighted)
        sh, sm, sl = split3(weighted * unit)
        alphas = placed_rows(split3(alpha), dims, width)
        for g, block in enumerate((fh, fm, sh, sm, alphas, fl, sl)):
            v_ref[g * dims:(g + 1) * dims, i * width:(i + 1) * width] = block.astype(bf16)

    col_count = plan.col_each * width
    grad = jnp.zeros((dims, width), jnp.float32)
    o_ref[plan.at_weight:, :] = jnp.zeros((LANES - plan.at_weight, width), jnp.float32)
    for i in range(plan.row_each):
        a_tile = a_ref[:, i * width:(i + 1) * width]

        def step(c, total):
            start = pl.multiple_of(c * STEP, STEP)
            exponent = jnp.dot(b_ref[pl.ds(start, STEP), :], a_tile, preferred_element_type=jnp.float32)
            kernel = jnp.exp2(exponent)
            high = kernel.astype(bf16)
            low = (kernel - high.astype(jnp.float32)).astype(bf16)
            from_high = jnp.dot(v_ref[:, pl.ds(start, STEP)], high, preferred_element_type=jnp.float32)
            from_low = jnp.dot(v_ref[:5 * dims, pl.ds(start, STEP)], low, preferred_element_type=jnp.float32)
            return total[0] + from_high, total[1] + from_low

        zeros = (jnp.zeros((7 * dims, width), jnp.float32), jnp.zeros((5 * dims, width), jnp.float32))
        big, small = lax.fori_loop(0, col_count // STEP, step, zeros, unroll=UNROLL)

        def part(x, g):
            return x[g * dims:(g + 1) * dims]

        first = (part(small, 0) + part(small, 1) + part(big, 5)) + part(big, 1) + part(big, 0)
        second = (part(small, 2) + part(small, 3) + part(big, 6)) + part(big, 3) + part(big, 2)
        weights = part(big, 4) + part(small, 4)
        weight = weights[0:1] + weights[1:2] + weights[2:3]
        unit = t_ref[i * dims:(i + 1) * dims, :]
        alpha = t_ref[plan.at_row_alpha + i:plan.at_row_alpha + i + 1, :]
        terms = 0.5 * alpha * (unit * unit * weight - 2.0 * unit * first + second)
        o_ref[i * dims:(i + 1) * dims, :] = terms
        o_ref[plan.at_weight + i:plan.at_weight + i + 1, :] = weight
        grad = grad + terms
    share = jnp.sum(grad, 1, keepdims=True)
    o_ref[plan.at_grad:plan.at_grad + dims, :] = jnp.broadcast_to(share, (dims, width))
    out_ref[...] = o_ref[...].T


def finish_kernel(plan, total_rows, in_ref, terms_ref, weight_ref, grad_ref):
    dims = plan.dims
    summed = jnp.sum(in_ref[...].reshape(plan.rows, plan.cols, LANES), 1)
    total = jnp.sum(summed, 0, keepdims=True)
    padded = jnp.concatenate([summed, jnp.zeros((LANES - plan.rows, LANES), jnp.float32)], 0)
    turned = padded.T
    terms = turned[:dims]
    weight = turned[plan.at_weight:plan.at_weight + 1]
    for i in range(1, plan.row_each):
        terms = terms + to_right(turned[i * dims:(i + 1) * dims], i * plan.rows)
        weight = weight + to_right(turned[plan.at_weight + i:plan.at_weight + i + 1], i * plan.rows)
    terms_ref[...] = terms
    weight_ref[...] = weight
    grad_ref[...] = to_left(total, plan.at_grad)[:, :dims] / total_rows


def on_device(x_rows, alpha_rows, x_cols, alpha_cols, lengthscale):
    dims, points = x_rows.shape
    devices = lax.axis_size(ROW_COL)
    plan = Plan(devices, dims, points)
    whole = pl.BlockSpec(memory_space=pltpu.VMEM)
    f32, bf16 = jnp.float32, jnp.bfloat16

    def exchanged(x, tiles):
        blocks = x.reshape(devices, 1, tiles * LANES)
        arrived = lax.all_to_all(blocks, ROW_COL, split_axis=0, concat_axis=0, tiled=True)
        return arrived.reshape(devices * tiles, LANES)

    blocks = pl.pallas_call(
        lambda *refs: spread_kernel(plan, *refs),
        out_shape=jax.ShapeDtypeStruct((devices * plan.tiles, LANES), f32),
        in_specs=[whole] * 5,
        out_specs=whole,
        compiler_params=pltpu.CompilerParams(vmem_limit_bytes=4 << 20),
        name="spread",
    )(x_rows, alpha_rows.reshape(1, points), x_cols, alpha_cols.reshape(1, points), lengthscale.reshape(1, dims))
    gathered = exchanged(blocks, plan.tiles)
    row_count, col_count = plan.row_each * devices, plan.col_each * devices
    shares = pl.pallas_call(
        lambda *refs: tile_kernel(plan, *refs),
        out_shape=jax.ShapeDtypeStruct((devices, LANES), f32),
        in_specs=[whole],
        out_specs=whole,
        scratch_shapes=[
            pltpu.VMEM((plan.tiles * LANES, devices), f32),
            pltpu.VMEM((8 * dims, row_count), bf16),
            pltpu.VMEM((col_count, 8 * dims), bf16),
            pltpu.VMEM((7 * dims, col_count), bf16),
            pltpu.VMEM((LANES, devices), f32),
        ],
        compiler_params=pltpu.CompilerParams(vmem_limit_bytes=16 << 20),
        name="tile",
    )(gathered)
    arrived = exchanged(shares, 1)
    terms, weight, grad = pl.pallas_call(
        lambda *refs: finish_kernel(plan, points * devices, *refs),
        out_shape=(
            jax.ShapeDtypeStruct((dims, points), f32),
            jax.ShapeDtypeStruct((1, points), f32),
            jax.ShapeDtypeStruct((1, dims), f32),
        ),
        in_specs=[whole],
        out_specs=(whole, whole, whole),
        compiler_params=pltpu.CompilerParams(vmem_limit_bytes=4 << 20),
        name="finish",
    )(arrived)
    return terms, weight.reshape(points), grad.reshape(dims)


def solution(mesh):
    finer = Mesh(mesh.devices.reshape(4, 2, 8, 4), ROW_COL)
    in_specs = (P(None, ROW_COL), P(ROW_COL), P(None, COL_ROW), P(COL_ROW), P())
    out_specs = (P(None, ROW_COL), P(ROW_COL), P())
    return jax.shard_map(on_device, mesh=finer, in_specs=in_specs, out_specs=out_specs, check_vma=False)
```

```python
import math

import jax
import jax.numpy as jnp
from jax import lax
from jax.experimental import pallas as pl
from jax.experimental.pallas import tpu as pltpu
from jax.sharding import Mesh
from jax.sharding import PartitionSpec as P

CORE = "row_1"
CHIPS = ("row_0", "col_0", "col_1")
CORE_CHIPS = (CORE, *CHIPS)
ROW_COL = ("row_0", "row_1", "col_0", "col_1")
COL_ROW = ("col_0", "col_1", "row_0", "row_1")
LOG2E = math.log2(math.e)
LANES = 128
COL_CLASSES = 8
STEP = 1024
OWN_STEP = 1024
ROW_TILE = 256


def split3(x):
    high = x.astype(jnp.bfloat16).astype(jnp.float32)
    rest = x - high
    middle = rest.astype(jnp.bfloat16).astype(jnp.float32)
    return high, middle, rest - middle


def placed_rows(entries, height, lanes):
    row = lax.broadcasted_iota(jnp.int32, (height, lanes), 0)
    block = jnp.zeros((height, lanes), jnp.float32)
    for k, entry in enumerate(entries):
        block = jnp.where(row == k, entry, block)
    return block


def to_left(x, lanes):
    return pltpu.roll(x, (LANES - lanes) % LANES, 1)


def to_right(x, lanes):
    return pltpu.roll(x, lanes % LANES, 1)


class Plan:
    def __init__(self, chips, dims, points):
        self.chips, self.devices, self.dims = chips, 2 * chips, dims
        self.cols = COL_CLASSES
        self.half = chips // self.cols
        self.rows = 2 * self.half
        self.row_each = points // self.rows
        self.col_each = points // self.cols
        self.of_rows = self.row_each * dims
        self.at_cols = 2 * self.of_rows
        self.at_col_alpha = self.at_cols + self.col_each * dims
        self.at_row_alpha = self.at_col_alpha + self.col_each
        self.tiles = pl.cdiv(self.at_row_alpha + 2 * self.row_each, LANES)
        self.at_weight = self.row_each * dims
        self.at_grad = self.at_weight + pl.cdiv(self.row_each, 8) * 8


def spread_kernel(plan, *refs):
    dims = plan.dims
    sources, out_ref, arrived, sems = refs[:5], refs[5], refs[6:11], refs[11]
    loads = [pltpu.make_async_copy(src, dst, sems.at[k]) for k, (src, dst) in enumerate(zip(sources, arrived))]
    for load in loads:
        load.start()
    for load in loads:
        load.wait()
    rows_ref, row_alpha_ref, cols_ref, col_alpha_ref, scale_ref = arrived
    scales = jnp.broadcast_to(scale_ref[:, :dims], (dims, dims))
    down = lax.broadcasted_iota(jnp.int32, (dims, dims), 0)
    along = lax.broadcasted_iota(jnp.int32, (dims, dims), 1)
    inverse = 1.0 / jnp.sum(jnp.where(down == along, scales, 0.0), 1, keepdims=True)
    rows = rows_ref[...] * inverse
    cols = cols_ref[...] * inverse
    of_class = [c * plan.half + i * plan.rows for c in range(2) for i in range(plan.row_each)]
    of_col = [i * plan.cols for i in range(plan.col_each)]
    pieces = [to_left(rows, k) for k in of_class] + [to_left(cols, k) for k in of_col]
    alphas = [to_left(col_alpha_ref[...], k) for k in of_col] + [to_left(row_alpha_ref[...], k) for k in of_class]
    pieces.append(placed_rows(alphas, plan.tiles * LANES - plan.at_col_alpha, LANES))
    stacked = jnp.concatenate(pieces, 0)
    for k in range(plan.tiles):
        turned = stacked[k * LANES:(k + 1) * LANES].T
        lane = lax.broadcasted_iota(jnp.int32, (plan.cols, LANES), 1) + k * LANES
        is_row = (lane < plan.at_cols) | (lane >= plan.at_row_alpha)
        of_cols = turned[:plan.cols]
        for r in range(plan.half):
            of_row = jnp.broadcast_to(turned[r:r + 1], (plan.cols, LANES))
            start = r * plan.cols * plan.tiles + k
            out_ref[pl.ds(start, plan.cols, stride=plan.tiles), :] = jnp.where(is_row, of_row, of_cols)


def prepared_exponents(unit, ones_first):
    dims, width = unit.shape
    scaled = unit * math.sqrt(LOG2E)
    norm = -0.5 * jnp.sum(scaled * scaled, 0, keepdims=True)
    parts = split3(norm)
    ones = (1.0, 1.0, 1.0)
    norms = placed_rows(ones + parts if ones_first else parts + ones, dims, width)
    h, m, l = split3(scaled)
    if ones_first:
        return h, m, h, m, l, h, norms, jnp.zeros_like(norms)
    return h, h, m, m, h, l, norms, jnp.zeros_like(norms)


def prepare(plan, in_ref, t_ref, b_ref, v_ref, a_ref):
    dims, width = plan.dims, plan.chips
    bf16 = jnp.bfloat16
    core = lax.axis_index(CORE)
    for k in range(plan.tiles):
        t_ref[k * LANES:(k + 1) * LANES, :] = in_ref[pl.ds(k, width, stride=plan.tiles), :].T
    for i in range(plan.row_each):
        unit = t_ref[pl.ds(pl.multiple_of(core * plan.of_rows, 8) + i * dims, dims), :]
        for g, block in enumerate(prepared_exponents(unit, False)):
            a_ref[g * dims:(g + 1) * dims, i * width:(i + 1) * width] = block.astype(bf16)
    for i in range(plan.col_each):
        at = plan.at_cols + i * dims
        unit = t_ref[at:at + dims, :]
        alpha = t_ref[plan.at_col_alpha + i:plan.at_col_alpha + i + 1, :]
        b_ref[i * width:(i + 1) * width, :] = jnp.concatenate(prepared_exponents(unit, True), 0).astype(bf16).T
        weighted = alpha * unit
        fh, fm, fl = split3(weighted)
        sh, sm, sl = split3(weighted * unit)
        alphas = placed_rows(split3(alpha), dims, width)
        for g, block in enumerate((fh, fm, sh, sm, alphas, fl, sl)):
            v_ref[g * dims:(g + 1) * dims, i * width:(i + 1) * width] = block.astype(bf16)


def add_columns(plan, sums, a_tiles, b_ref, v_ref, step):
    f32, bf16 = jnp.float32, jnp.bfloat16
    sums = list(sums)
    for start in range(0, b_ref.shape[0], step):
        points = b_ref[start:start + step, :]
        values = v_ref[:, start:start + step]
        kernels = [jnp.exp2(jnp.dot(points, a_tile, preferred_element_type=f32)) for a_tile in a_tiles]
        highs = [kernel.astype(bf16) for kernel in kernels]
        lows = [(kernel - high.astype(f32)).astype(bf16) for kernel, high in zip(kernels, highs)]
        bigs = [jnp.dot(values, high, preferred_element_type=f32) for high in highs]
        smalls = [jnp.dot(values[:5 * plan.dims], low, preferred_element_type=f32) for low in lows]
        sums = [(s[0] + big, s[1] + small) for s, big, small in zip(sums, bigs, smalls)]
    return sums


def zero_sums(plan):
    return jnp.zeros((7 * plan.dims, ROW_TILE), jnp.float32), jnp.zeros((5 * plan.dims, ROW_TILE), jnp.float32)


def own_kernel(plan, own_ref, t_ref, b_ref, v_ref, a_ref, big_ref, small_ref):
    prepare(plan, own_ref, t_ref, b_ref, v_ref, a_ref)
    cuts = row_cuts(a_ref)
    sums = add_columns(plan, [zero_sums(plan)] * len(cuts), [a_ref[:, cut] for cut in cuts], b_ref, v_ref, OWN_STEP)
    for cut, (big, small) in zip(cuts, sums):
        big_ref[:, cut], small_ref[:, cut] = big, small


def row_cuts(a_ref):
    return [slice(start, start + ROW_TILE) for start in range(0, a_ref.shape[1], ROW_TILE)]


def tile_kernel(plan, other_ref, own_t_ref, own_b_ref, own_v_ref, own_a_ref, big_ref, small_ref, out_ref, t_ref, b_ref, v_ref, a_ref, o_ref):
    dims, width = plan.dims, plan.chips
    prepare(plan, other_ref, t_ref, b_ref, v_ref, a_ref)
    core = lax.axis_index(CORE)
    grad = jnp.zeros((dims, width), jnp.float32)
    o_ref[plan.at_weight:, :] = jnp.zeros((LANES - plan.at_weight, 2 * width), jnp.float32)
    for points_ref, rows_ref, place in ((own_t_ref, own_a_ref, core), (t_ref, a_ref, 1 - core)):
        lanes = pl.ds(pl.multiple_of(place * width, LANES), width)
        cuts = row_cuts(rows_ref)
        a_tiles = [rows_ref[:, cut] for cut in cuts]
        if rows_ref is own_a_ref:
            sums = [(big_ref[:, cut], small_ref[:, cut]) for cut in cuts]
        else:
            sums = add_columns(plan, [zero_sums(plan)] * len(cuts), a_tiles, own_b_ref, own_v_ref, STEP)
        sums = add_columns(plan, sums, a_tiles, b_ref, v_ref, STEP)
        for cut, (big, small) in zip(cuts, sums):
            start = cut.start

            def part(x, g):
                return x[g * dims:(g + 1) * dims]

            first = (part(small, 0) + part(small, 1) + part(big, 5)) + part(big, 1) + part(big, 0)
            second = (part(small, 2) + part(small, 3) + part(big, 6)) + part(big, 3) + part(big, 2)
            weights = part(big, 4) + part(small, 4)
            weight = weights[0:1] + weights[1:2] + weights[2:3]
            for i in range(start // width, (start + ROW_TILE) // width):
                cut = slice(i * width - start, (i + 1) * width - start)
                unit = points_ref[pl.ds(pl.multiple_of(core * plan.of_rows, 8) + i * dims, dims), :]
                alpha = points_ref[pl.ds(plan.at_row_alpha + core * plan.row_each + i, 1), :]
                terms = 0.5 * alpha * (unit * unit * weight[:, cut] - 2.0 * unit * first[:, cut] + second[:, cut])
                o_ref[i * dims:(i + 1) * dims, lanes] = terms
                o_ref[plan.at_weight + i:plan.at_weight + i + 1, lanes] = weight[:, cut]
                grad = grad + terms
    share = jnp.sum(grad, 1, keepdims=True)
    o_ref[plan.at_grad:plan.at_grad + dims, :] = jnp.broadcast_to(share, (dims, 2 * width))
    out_ref[...] = o_ref[...].T


def finish_kernel(plan, total_rows, in_ref, terms_ref, weight_ref, grad_ref):
    dims = plan.dims
    summed = jnp.sum(in_ref[...].reshape(plan.rows, plan.cols, LANES), 1)
    total = jnp.sum(summed, 0, keepdims=True)
    padded = jnp.concatenate([summed, jnp.zeros((LANES - plan.rows, LANES), jnp.float32)], 0)
    turned = padded.T
    terms = turned[:dims]
    weight = turned[plan.at_weight:plan.at_weight + 1]
    for i in range(1, plan.row_each):
        terms = terms + to_right(turned[i * dims:(i + 1) * dims], i * plan.rows)
        weight = weight + to_right(turned[plan.at_weight + i:plan.at_weight + i + 1], i * plan.rows)
    terms_ref[...] = terms
    weight_ref[...] = weight
    grad_ref[...] = to_left(total, plan.at_grad)[:, :dims] / total_rows


def on_device(x_rows, alpha_rows, x_cols, alpha_cols, lengthscale):
    dims, points = x_rows.shape
    chips = lax.axis_size(CHIPS)
    devices = 2 * chips
    plan = Plan(chips, dims, points)
    whole = pl.BlockSpec(memory_space=pltpu.VMEM)
    f32, bf16 = jnp.float32, jnp.bfloat16

    def exchanged(x, axes):
        blocks = x.reshape(lax.axis_size(axes), 1, -1)
        return lax.all_to_all(blocks, axes, split_axis=0, concat_axis=0, tiled=True).reshape(x.shape)

    sources = (x_rows, alpha_rows.reshape(1, points), x_cols, alpha_cols.reshape(1, points), lengthscale.reshape(1, dims))
    blocks = pl.pallas_call(
        lambda *refs: spread_kernel(plan, *refs),
        out_shape=jax.ShapeDtypeStruct((chips * plan.tiles, LANES), f32),
        in_specs=[pl.BlockSpec(memory_space=pltpu.HBM)] * 5,
        out_specs=whole,
        scratch_shapes=[
            pltpu.VMEM((dims, points), f32),
            pltpu.VMEM((1, points), f32),
            pltpu.VMEM((dims, points), f32),
            pltpu.VMEM((1, points), f32),
            pltpu.VMEM((1, dims), f32),
            pltpu.SemaphoreType.DMA((5,)),
        ],
        compiler_params=pltpu.CompilerParams(vmem_limit_bytes=4 << 20),
        name="spread",
    )(*(pltpu.with_memory_space_constraint(x, pltpu.HBM) for x in sources))
    own = exchanged(blocks, CHIPS)
    other = lax.ppermute(own, CORE, [(0, 1), (1, 0)])
    row_half, col_half = plan.row_each * chips, plan.col_each * chips
    prepared = (
        jax.ShapeDtypeStruct((plan.tiles * LANES, chips), f32),
        jax.ShapeDtypeStruct((col_half, 8 * dims), bf16),
        jax.ShapeDtypeStruct((7 * dims, col_half), bf16),
        jax.ShapeDtypeStruct((8 * dims, row_half), bf16),
    )
    sums = (
        jax.ShapeDtypeStruct((7 * dims, row_half), f32),
        jax.ShapeDtypeStruct((5 * dims, row_half), f32),
    )
    own_parts = pl.pallas_call(
        lambda *refs: own_kernel(plan, *refs),
        out_shape=prepared + sums,
        in_specs=[whole],
        out_specs=(whole,) * 6,
        compiler_params=pltpu.CompilerParams(vmem_limit_bytes=12 << 20),
        cost_estimate=pl.CostEstimate(flops=2 << 30, bytes_accessed=1 << 20, transcendentals=0),
        name="own",
    )(own)
    shares = pl.pallas_call(
        lambda *refs: tile_kernel(plan, *refs),
        out_shape=jax.ShapeDtypeStruct((devices, LANES), f32),
        in_specs=[whole] * 7,
        out_specs=whole,
        scratch_shapes=[
            *(pltpu.VMEM(part.shape, part.dtype) for part in prepared),
            pltpu.VMEM((LANES, devices), f32),
        ],
        compiler_params=pltpu.CompilerParams(vmem_limit_bytes=16 << 20),
        name="tile",
    )(other, *own_parts)
    arrived = exchanged(shares, CORE_CHIPS)
    terms, weight, grad = pl.pallas_call(
        lambda *refs: finish_kernel(plan, points * devices, *refs),
        out_shape=(
            jax.ShapeDtypeStruct((dims, points), f32),
            jax.ShapeDtypeStruct((1, points), f32),
            jax.ShapeDtypeStruct((1, dims), f32),
        ),
        in_specs=[whole],
        out_specs=(whole, whole, whole),
        compiler_params=pltpu.CompilerParams(vmem_limit_bytes=4 << 20),
        name="finish",
    )(arrived)
    return terms, weight.reshape(points), grad.reshape(dims)


def solution(mesh):
    finer = Mesh(mesh.devices.reshape(4, 2, 8, 4), ROW_COL)
    in_specs = (P(None, ROW_COL), P(ROW_COL), P(None, COL_ROW), P(COL_ROW), P())
    out_specs = (P(None, ROW_COL), P(ROW_COL), P())
    return jax.shard_map(on_device, mesh=finer, in_specs=in_specs, out_specs=out_specs, check_vma=False)
```

```python
import math

import jax
import jax.numpy as jnp
from jax import lax
from jax.experimental import pallas as pl
from jax.experimental.pallas import tpu as pltpu
from jax.sharding import Mesh
from jax.sharding import PartitionSpec as P

CORE = "row_1"
CHIPS = ("row_0", "col_0", "col_1")
CHIPS_CORE = (*CHIPS, CORE)
ROW_COL = ("row_0", "row_1", "col_0", "col_1")
COL_ROW = ("col_0", "col_1", "row_0", "row_1")
LOG2E = math.log2(math.e)
LANES = 128
COL_CLASSES = 8
STEP = 1024
OWN_STEP = 1024
ROW_TILE = 256


def split3(x):
    high = x.astype(jnp.bfloat16).astype(jnp.float32)
    rest = x - high
    middle = rest.astype(jnp.bfloat16).astype(jnp.float32)
    return high, middle, rest - middle


def placed_rows(entries, height, lanes):
    row = lax.broadcasted_iota(jnp.int32, (height, lanes), 0)
    block = jnp.zeros((height, lanes), jnp.float32)
    for k, entry in enumerate(entries):
        block = jnp.where(row == k, entry, block)
    return block


def to_left(x, lanes):
    return pltpu.roll(x, (LANES - lanes) % LANES, 1)


def to_right(x, lanes):
    return pltpu.roll(x, lanes % LANES, 1)


class Plan:
    def __init__(self, chips, dims, points):
        self.chips, self.devices, self.dims = chips, 2 * chips, dims
        self.cols = COL_CLASSES
        self.half = chips // self.cols
        self.rows = 2 * self.half
        self.row_each = points // self.rows
        self.col_each = points // self.cols
        self.of_rows = self.row_each * dims
        self.at_cols = 2 * self.of_rows
        self.at_col_alpha = self.at_cols + self.col_each * dims
        self.at_row_alpha = self.at_col_alpha + self.col_each
        self.tiles = pl.cdiv(self.at_row_alpha + 2 * self.row_each, LANES)
        self.at_weight = self.row_each * dims
        self.at_grad = self.at_weight + pl.cdiv(self.row_each, 8) * 8


def spread_kernel(plan, *refs):
    dims = plan.dims
    sources, out_ref, arrived, sems = refs[:5], refs[5], refs[6:11], refs[11]
    loads = [pltpu.make_async_copy(src, dst, sems.at[k]) for k, (src, dst) in enumerate(zip(sources, arrived))]
    for load in loads:
        load.start()
    for load in loads:
        load.wait()
    rows_ref, row_alpha_ref, cols_ref, col_alpha_ref, scale_ref = arrived
    scales = jnp.broadcast_to(scale_ref[:, :dims], (dims, dims))
    down = lax.broadcasted_iota(jnp.int32, (dims, dims), 0)
    along = lax.broadcasted_iota(jnp.int32, (dims, dims), 1)
    inverse = 1.0 / jnp.sum(jnp.where(down == along, scales, 0.0), 1, keepdims=True)
    rows = rows_ref[...] * inverse
    cols = cols_ref[...] * inverse
    of_class = [c * plan.half + i * plan.rows for c in range(2) for i in range(plan.row_each)]
    of_col = [i * plan.cols for i in range(plan.col_each)]
    pieces = [to_left(rows, k) for k in of_class] + [to_left(cols, k) for k in of_col]
    alphas = [to_left(col_alpha_ref[...], k) for k in of_col] + [to_left(row_alpha_ref[...], k) for k in of_class]
    pieces.append(placed_rows(alphas, plan.tiles * LANES - plan.at_col_alpha, LANES))
    stacked = jnp.concatenate(pieces, 0)
    for k in range(plan.tiles):
        turned = stacked[k * LANES:(k + 1) * LANES].T
        lane = lax.broadcasted_iota(jnp.int32, (plan.cols, LANES), 1) + k * LANES
        is_row = (lane < plan.at_cols) | (lane >= plan.at_row_alpha)
        of_cols = turned[:plan.cols]
        for r in range(plan.half):
            of_row = jnp.broadcast_to(turned[r:r + 1], (plan.cols, LANES))
            start = r * plan.cols * plan.tiles + k
            out_ref[pl.ds(start, plan.cols, stride=plan.tiles), :] = jnp.where(is_row, of_row, of_cols)


def prepared_exponents(unit, ones_first):
    dims, width = unit.shape
    scaled = unit * math.sqrt(LOG2E)
    norm = -0.5 * jnp.sum(scaled * scaled, 0, keepdims=True)
    parts = split3(norm)
    ones = (1.0, 1.0, 1.0)
    norms = placed_rows(ones + parts if ones_first else parts + ones, dims, width)
    h, m, l = split3(scaled)
    if ones_first:
        return h, m, h, m, l, h, norms, jnp.zeros_like(norms)
    return h, h, m, m, h, l, norms, jnp.zeros_like(norms)


def prepare_rows(plan, in_ref, t_ref, a_ref):
    dims, width = plan.dims, plan.chips
    bf16 = jnp.bfloat16
    core = lax.axis_index(CORE)
    for k in range(plan.tiles):
        t_ref[k * LANES:(k + 1) * LANES, :] = in_ref[pl.ds(k, width, stride=plan.tiles), :].T
    for i in range(plan.row_each):
        unit = t_ref[pl.ds(pl.multiple_of(core * plan.of_rows, 8) + i * dims, dims), :]
        for g, block in enumerate(prepared_exponents(unit, False)):
            a_ref[g * dims:(g + 1) * dims, i * width:(i + 1) * width] = block.astype(bf16)


def prepare_cols(plan, t_ref, b_ref, v_ref):
    dims, width = plan.dims, plan.chips
    bf16 = jnp.bfloat16
    for i in range(plan.col_each):
        at = plan.at_cols + i * dims
        unit = t_ref[at:at + dims, :]
        alpha = t_ref[plan.at_col_alpha + i:plan.at_col_alpha + i + 1, :]
        b_ref[i * width:(i + 1) * width, :] = jnp.concatenate(prepared_exponents(unit, True), 0).astype(bf16).T
        weighted = alpha * unit
        fh, fm, fl = split3(weighted)
        sh, sm, sl = split3(weighted * unit)
        alphas = placed_rows(split3(alpha), dims, width)
        for g, block in enumerate((fh, fm, sh, sm, alphas, fl, sl)):
            v_ref[g * dims:(g + 1) * dims, i * width:(i + 1) * width] = block.astype(bf16)


def add_columns(plan, sums, a_tiles, b_ref, v_ref, step):
    f32, bf16 = jnp.float32, jnp.bfloat16
    sums = list(sums)
    for start in range(0, b_ref.shape[0], step):
        points = b_ref[start:start + step, :]
        values = v_ref[:, start:start + step]
        kernels = [jnp.exp2(jnp.dot(points, a_tile, preferred_element_type=f32)) for a_tile in a_tiles]
        highs = [kernel.astype(bf16) for kernel in kernels]
        lows = [(kernel - high.astype(f32)).astype(bf16) for kernel, high in zip(kernels, highs)]
        bigs = [jnp.dot(values, high, preferred_element_type=f32) for high in highs]
        smalls = [jnp.dot(values[:5 * plan.dims], low, preferred_element_type=f32) for low in lows]
        sums = [(s[0] + big, s[1] + small) for s, big, small in zip(sums, bigs, smalls)]
    return sums


def zero_sums(plan):
    return jnp.zeros((7 * plan.dims, ROW_TILE), jnp.float32), jnp.zeros((5 * plan.dims, ROW_TILE), jnp.float32)


def own_kernel(plan, own_ref, t_ref, b_ref, v_ref, a_ref, big_ref, small_ref):
    prepare_rows(plan, own_ref, t_ref, a_ref)
    prepare_cols(plan, t_ref, b_ref, v_ref)
    cuts = row_cuts(a_ref)
    for cut in cuts:
        (big, small), = add_columns(plan, [zero_sums(plan)], [a_ref[:, cut]], b_ref, v_ref, OWN_STEP)
        big_ref[:, cut], small_ref[:, cut] = big, small


def row_cuts(a_ref):
    return [slice(start, start + ROW_TILE) for start in range(0, a_ref.shape[1], ROW_TILE)]


def tile_kernel(plan, other_ref, own_t_ref, own_b_ref, own_v_ref, own_a_ref, big_ref, small_ref, out_ref, t_ref, b_ref, v_ref, a_ref, o_ref):
    dims, width = plan.dims, plan.chips
    prepare_rows(plan, other_ref, t_ref, a_ref)
    cuts = row_cuts(a_ref)
    other_sums = add_columns(plan, [zero_sums(plan)] * len(cuts), [a_ref[:, cut] for cut in cuts], own_b_ref, own_v_ref, STEP)
    prepare_cols(plan, t_ref, b_ref, v_ref)
    core = lax.axis_index(CORE)
    grad = jnp.zeros((dims, width), jnp.float32)
    o_ref[plan.at_weight:, :] = jnp.zeros((LANES - plan.at_weight, 2 * width), jnp.float32)
    for points_ref, rows_ref, place in ((own_t_ref, own_a_ref, core), (t_ref, a_ref, 1 - core)):
        lanes = pl.ds(pl.multiple_of(place * width, LANES), width)
        cuts = row_cuts(rows_ref)
        a_tiles = [rows_ref[:, cut] for cut in cuts]
        if rows_ref is own_a_ref:
            sums = [(big_ref[:, cut], small_ref[:, cut]) for cut in cuts]
        else:
            sums = other_sums
        sums = add_columns(plan, sums, a_tiles, b_ref, v_ref, STEP)
        for cut, (big, small) in zip(cuts, sums):
            start = cut.start

            def part(x, g):
                return x[g * dims:(g + 1) * dims]

            first = (part(small, 0) + part(small, 1) + part(big, 5)) + part(big, 1) + part(big, 0)
            second = (part(small, 2) + part(small, 3) + part(big, 6)) + part(big, 3) + part(big, 2)
            weights = part(big, 4) + part(small, 4)
            weight = weights[0:1] + weights[1:2] + weights[2:3]
            for i in range(start // width, (start + ROW_TILE) // width):
                cut = slice(i * width - start, (i + 1) * width - start)
                unit = points_ref[pl.ds(pl.multiple_of(core * plan.of_rows, 8) + i * dims, dims), :]
                alpha = points_ref[pl.ds(plan.at_row_alpha + core * plan.row_each + i, 1), :]
                terms = 0.5 * alpha * (unit * unit * weight[:, cut] - 2.0 * unit * first[:, cut] + second[:, cut])
                o_ref[i * dims:(i + 1) * dims, lanes] = terms
                o_ref[plan.at_weight + i:plan.at_weight + i + 1, lanes] = weight[:, cut]
                grad = grad + terms
    share = jnp.sum(grad, 1, keepdims=True)
    o_ref[plan.at_grad:plan.at_grad + dims, :] = jnp.broadcast_to(share, (dims, 2 * width))
    for place in range(2):
        out_ref[pl.ds(place, width, stride=2), :] = o_ref[:, place * width:(place + 1) * width].T


def finish_kernel(plan, total_rows, in_ref, terms_ref, weight_ref, grad_ref):
    dims = plan.dims
    by_core = [in_ref[pl.ds(core, plan.chips, stride=2), :] for core in range(2)]
    summed = jnp.concatenate([jnp.sum(x.reshape(plan.half, plan.cols, LANES), 1) for x in by_core], 0)
    total = jnp.sum(summed, 0, keepdims=True)
    padded = jnp.concatenate([summed, jnp.zeros((LANES - plan.rows, LANES), jnp.float32)], 0)
    turned = padded.T
    terms = turned[:dims]
    weight = turned[plan.at_weight:plan.at_weight + 1]
    for i in range(1, plan.row_each):
        terms = terms + to_right(turned[i * dims:(i + 1) * dims], i * plan.rows)
        weight = weight + to_right(turned[plan.at_weight + i:plan.at_weight + i + 1], i * plan.rows)
    terms_ref[...] = terms
    weight_ref[...] = weight
    grad_ref[...] = to_left(total, plan.at_grad)[:, :dims] / total_rows


def on_device(x_rows, alpha_rows, x_cols, alpha_cols, lengthscale):
    dims, points = x_rows.shape
    chips = lax.axis_size(CHIPS)
    devices = 2 * chips
    plan = Plan(chips, dims, points)
    whole = pl.BlockSpec(memory_space=pltpu.VMEM)
    f32, bf16 = jnp.float32, jnp.bfloat16

    def exchanged(x, axes):
        blocks = x.reshape(lax.axis_size(axes), 1, -1)
        return lax.all_to_all(blocks, axes, split_axis=0, concat_axis=0, tiled=True).reshape(x.shape)

    sources = (x_rows, alpha_rows.reshape(1, points), x_cols, alpha_cols.reshape(1, points), lengthscale.reshape(1, dims))
    blocks = pl.pallas_call(
        lambda *refs: spread_kernel(plan, *refs),
        out_shape=jax.ShapeDtypeStruct((chips * plan.tiles, LANES), f32),
        in_specs=[pl.BlockSpec(memory_space=pltpu.HBM)] * 5,
        out_specs=whole,
        scratch_shapes=[
            pltpu.VMEM((dims, points), f32),
            pltpu.VMEM((1, points), f32),
            pltpu.VMEM((dims, points), f32),
            pltpu.VMEM((1, points), f32),
            pltpu.VMEM((1, dims), f32),
            pltpu.SemaphoreType.DMA((5,)),
        ],
        compiler_params=pltpu.CompilerParams(vmem_limit_bytes=4 << 20),
        name="spread",
    )(*(pltpu.with_memory_space_constraint(x, pltpu.HBM) for x in sources))
    own = exchanged(blocks, CHIPS)
    other = lax.ppermute(own, CORE, [(0, 1), (1, 0)])
    row_half, col_half = plan.row_each * chips, plan.col_each * chips
    prepared = (
        jax.ShapeDtypeStruct((plan.tiles * LANES, chips), f32),
        jax.ShapeDtypeStruct((col_half, 8 * dims), bf16),
        jax.ShapeDtypeStruct((7 * dims, col_half), bf16),
        jax.ShapeDtypeStruct((8 * dims, row_half), bf16),
    )
    sums = (
        jax.ShapeDtypeStruct((7 * dims, row_half), f32),
        jax.ShapeDtypeStruct((5 * dims, row_half), f32),
    )
    own_parts = pl.pallas_call(
        lambda *refs: own_kernel(plan, *refs),
        out_shape=prepared + sums,
        in_specs=[whole],
        out_specs=(whole,) * 6,
        compiler_params=pltpu.CompilerParams(vmem_limit_bytes=12 << 20),
        cost_estimate=pl.CostEstimate(flops=2 << 30, bytes_accessed=1 << 20, transcendentals=0),
        name="own",
    )(own)
    shares = pl.pallas_call(
        lambda *refs: tile_kernel(plan, *refs),
        out_shape=jax.ShapeDtypeStruct((devices, LANES), f32),
        in_specs=[whole] * 7,
        out_specs=whole,
        scratch_shapes=[
            *(pltpu.VMEM(part.shape, part.dtype) for part in prepared),
            pltpu.VMEM((LANES, devices), f32),
        ],
        compiler_params=pltpu.CompilerParams(vmem_limit_bytes=16 << 20),
        name="tile",
    )(other, *own_parts)
    arrived = exchanged(shares, CHIPS_CORE)
    terms, weight, grad = pl.pallas_call(
        lambda *refs: finish_kernel(plan, points * devices, *refs),
        out_shape=(
            jax.ShapeDtypeStruct((dims, points), f32),
            jax.ShapeDtypeStruct((1, points), f32),
            jax.ShapeDtypeStruct((1, dims), f32),
        ),
        in_specs=[whole],
        out_specs=(whole, whole, whole),
        compiler_params=pltpu.CompilerParams(vmem_limit_bytes=4 << 20),
        name="finish",
    )(arrived)
    return terms, weight.reshape(points), grad.reshape(dims)


def solution(mesh):
    finer = Mesh(mesh.devices.reshape(4, 2, 8, 4), ROW_COL)
    in_specs = (P(None, ROW_COL), P(ROW_COL), P(None, COL_ROW), P(COL_ROW), P())
    out_specs = (P(None, ROW_COL), P(ROW_COL), P())
    return jax.shard_map(on_device, mesh=finer, in_specs=in_specs, out_specs=out_specs, check_vma=False)
```

```python
import math

import jax
import jax.numpy as jnp
from jax import lax
from jax.experimental import pallas as pl
from jax.experimental.pallas import tpu as pltpu
from jax.sharding import Mesh
from jax.sharding import PartitionSpec as P

CORE = "row_1"
CHIPS = ("row_0", "col_0", "col_1")
CHIPS_CORE = (*CHIPS, CORE)
ROW_COL = ("row_0", "row_1", "col_0", "col_1")
COL_ROW = ("col_0", "col_1", "row_0", "row_1")
LOG2E = math.log2(math.e)
LANES = 128
COL_CLASSES = 8
STEP = 1024
ROW_TILE = 256


def split3(x):
    high = x.astype(jnp.bfloat16).astype(jnp.float32)
    rest = x - high
    middle = rest.astype(jnp.bfloat16).astype(jnp.float32)
    return high, middle, rest - middle


def placed_rows(entries, height, lanes):
    row = lax.broadcasted_iota(jnp.int32, (height, lanes), 0)
    block = jnp.zeros((height, lanes), jnp.float32)
    for k, entry in enumerate(entries):
        block = jnp.where(row == k, entry, block)
    return block


def to_left(x, lanes):
    return pltpu.roll(x, (LANES - lanes) % LANES, 1)


def to_right(x, lanes):
    return pltpu.roll(x, lanes % LANES, 1)


class Plan:
    def __init__(self, chips, dims, points):
        self.chips, self.devices, self.dims = chips, 2 * chips, dims
        self.cols = COL_CLASSES
        self.half = chips // self.cols
        self.rows = 2 * self.half
        self.row_each = points // self.rows
        self.col_each = points // self.cols
        self.of_rows = self.row_each * dims
        self.at_cols = 2 * self.of_rows
        self.at_col_alpha = self.at_cols + self.col_each * dims
        self.at_row_alpha = self.at_col_alpha + self.col_each
        self.tiles = pl.cdiv(self.at_row_alpha + 2 * self.row_each, LANES)
        self.at_weight = self.row_each * dims
        self.at_grad = self.at_weight + pl.cdiv(self.row_each, 8) * 8


def spread_kernel(plan, *refs):
    dims = plan.dims
    sources, out_ref, arrived, sems = refs[:5], refs[5], refs[6:11], refs[11]
    loads = [pltpu.make_async_copy(src, dst, sems.at[k]) for k, (src, dst) in enumerate(zip(sources, arrived))]
    for load in loads:
        load.start()
    for load in loads:
        load.wait()
    rows_ref, row_alpha_ref, cols_ref, col_alpha_ref, scale_ref = arrived
    scales = jnp.broadcast_to(scale_ref[:, :dims], (dims, dims))
    down = lax.broadcasted_iota(jnp.int32, (dims, dims), 0)
    along = lax.broadcasted_iota(jnp.int32, (dims, dims), 1)
    inverse = 1.0 / jnp.sum(jnp.where(down == along, scales, 0.0), 1, keepdims=True)
    rows = rows_ref[...] * inverse
    cols = cols_ref[...] * inverse
    of_class = [c * plan.half + i * plan.rows for c in range(2) for i in range(plan.row_each)]
    of_col = [i * plan.cols for i in range(plan.col_each)]
    pieces = [to_left(rows, k) for k in of_class] + [to_left(cols, k) for k in of_col]
    alphas = [to_left(col_alpha_ref[...], k) for k in of_col] + [to_left(row_alpha_ref[...], k) for k in of_class]
    pieces.append(placed_rows(alphas, plan.tiles * LANES - plan.at_col_alpha, LANES))
    stacked = jnp.concatenate(pieces, 0)
    for k in range(plan.tiles):
        turned = stacked[k * LANES:(k + 1) * LANES].T
        lane = lax.broadcasted_iota(jnp.int32, (plan.cols, LANES), 1) + k * LANES
        is_row = (lane < plan.at_cols) | (lane >= plan.at_row_alpha)
        of_cols = turned[:plan.cols]
        for r in range(plan.half):
            of_row = jnp.broadcast_to(turned[r:r + 1], (plan.cols, LANES))
            start = r * plan.cols * plan.tiles + k
            out_ref[pl.ds(start, plan.cols, stride=plan.tiles), :] = jnp.where(is_row, of_row, of_cols)


def prepared_exponents(unit, ones_first):
    dims, width = unit.shape
    scaled = unit * math.sqrt(LOG2E)
    norm = -0.5 * jnp.sum(scaled * scaled, 0, keepdims=True)
    parts = split3(norm)
    ones = (1.0, 1.0, 1.0)
    norms = placed_rows(ones + parts if ones_first else parts + ones, dims, width)
    h, m, l = split3(scaled)
    if ones_first:
        return h, m, h, m, l, h, norms, jnp.zeros_like(norms)
    return h, h, m, m, h, l, norms, jnp.zeros_like(norms)


def prepare_rows(plan, in_ref, t_ref, a_ref):
    dims, width = plan.dims, plan.chips
    bf16 = jnp.bfloat16
    core = lax.axis_index(CORE)
    for k in range(plan.tiles):
        t_ref[k * LANES:(k + 1) * LANES, :] = in_ref[pl.ds(k, width, stride=plan.tiles), :].T
    for i in range(plan.row_each):
        unit = t_ref[pl.ds(pl.multiple_of(core * plan.of_rows, 8) + i * dims, dims), :]
        for g, block in enumerate(prepared_exponents(unit, False)):
            a_ref[g * dims:(g + 1) * dims, i * width:(i + 1) * width] = block.astype(bf16)


def prepare_cols(plan, t_ref, b_ref, v_ref):
    dims, width = plan.dims, plan.chips
    bf16 = jnp.bfloat16
    for i in range(plan.col_each):
        at = plan.at_cols + i * dims
        unit = t_ref[at:at + dims, :]
        alpha = t_ref[plan.at_col_alpha + i:plan.at_col_alpha + i + 1, :]
        b_ref[i * width:(i + 1) * width, :] = jnp.concatenate(prepared_exponents(unit, True), 0).astype(bf16).T
        weighted = alpha * unit
        fh, fm, fl = split3(weighted)
        sh, sm, sl = split3(weighted * unit)
        alphas = placed_rows(split3(alpha), dims, width)
        for g, block in enumerate((fh, fm, sh, sm, alphas, fl, sl)):
            v_ref[g * dims:(g + 1) * dims, i * width:(i + 1) * width] = block.astype(bf16)


def add_columns(plan, sums, a_tiles, b_ref, v_ref, step):
    f32, bf16 = jnp.float32, jnp.bfloat16
    sums = list(sums)
    for start in range(0, b_ref.shape[0], step):
        points = b_ref[start:start + step, :]
        values = v_ref[:, start:start + step]
        kernels = [jnp.exp2(jnp.dot(points, a_tile, preferred_element_type=f32)) for a_tile in a_tiles]
        highs = [kernel.astype(bf16) for kernel in kernels]
        lows = [(kernel - high.astype(f32)).astype(bf16) for kernel, high in zip(kernels, highs)]
        bigs = [jnp.dot(values, high, preferred_element_type=f32) for high in highs]
        smalls = [jnp.dot(values[:5 * plan.dims], low, preferred_element_type=f32) for low in lows]
        sums = [(s[0] + big, s[1] + small) for s, big, small in zip(sums, bigs, smalls)]
    return sums


def zero_sums(plan):
    return jnp.zeros((7 * plan.dims, ROW_TILE), jnp.float32), jnp.zeros((5 * plan.dims, ROW_TILE), jnp.float32)


def own_kernel(plan, own_ref, t_ref, b_ref, v_ref, a_ref, big_ref, small_ref):
    prepare_rows(plan, own_ref, t_ref, a_ref)
    prepare_cols(plan, t_ref, b_ref, v_ref)
    cuts = row_cuts(a_ref)
    for cut in cuts:
        (big, small), = add_columns(plan, [zero_sums(plan)], [a_ref[:, cut]], b_ref, v_ref, STEP)
        big_ref[:, cut], small_ref[:, cut] = big, small


def row_cuts(a_ref):
    return [slice(start, start + ROW_TILE) for start in range(0, a_ref.shape[1], ROW_TILE)]


def tile_kernel(plan, other_ref, own_t_ref, own_b_ref, own_v_ref, own_a_ref, big_ref, small_ref, out_ref, t_ref, b_ref, v_ref, a_ref, o_ref):
    dims, width = plan.dims, plan.chips
    prepare_rows(plan, other_ref, t_ref, a_ref)
    cuts = row_cuts(a_ref)
    other_sums = add_columns(plan, [zero_sums(plan)] * len(cuts), [a_ref[:, cut] for cut in cuts], own_b_ref, own_v_ref, STEP)
    prepare_cols(plan, t_ref, b_ref, v_ref)
    core = lax.axis_index(CORE)
    grad = jnp.zeros((dims, width), jnp.float32)
    o_ref[plan.at_weight:, :] = jnp.zeros((LANES - plan.at_weight, 2 * width), jnp.float32)
    tiles = [(own_t_ref, own_a_ref, cut, core) for cut in cuts] + [(t_ref, a_ref, cut, 1 - core) for cut in cuts]
    sums = [(big_ref[:, cut], small_ref[:, cut]) for cut in cuts] + other_sums
    sums = add_columns(plan, sums, [rows_ref[:, cut] for _, rows_ref, cut, _ in tiles], b_ref, v_ref, STEP)
    for (points_ref, _, cut, place), (big, small) in zip(tiles, sums):
        lanes = pl.ds(pl.multiple_of(place * width, LANES), width)
        start = cut.start

        def part(x, g):
            return x[g * dims:(g + 1) * dims]

        first = (part(small, 0) + part(small, 1) + part(big, 5)) + part(big, 1) + part(big, 0)
        second = (part(small, 2) + part(small, 3) + part(big, 6)) + part(big, 3) + part(big, 2)
        weights = part(big, 4) + part(small, 4)
        weight = weights[0:1] + weights[1:2] + weights[2:3]
        for i in range(start // width, (start + ROW_TILE) // width):
            cut = slice(i * width - start, (i + 1) * width - start)
            unit = points_ref[pl.ds(pl.multiple_of(core * plan.of_rows, 8) + i * dims, dims), :]
            alpha = points_ref[pl.ds(plan.at_row_alpha + core * plan.row_each + i, 1), :]
            terms = 0.5 * alpha * (unit * unit * weight[:, cut] - 2.0 * unit * first[:, cut] + second[:, cut])
            o_ref[i * dims:(i + 1) * dims, lanes] = terms
            o_ref[plan.at_weight + i:plan.at_weight + i + 1, lanes] = weight[:, cut]
            grad = grad + terms
    share = jnp.sum(grad, 1, keepdims=True)
    o_ref[plan.at_grad:plan.at_grad + dims, :] = jnp.broadcast_to(share, (dims, 2 * width))
    for place in range(2):
        out_ref[pl.ds(place, width, stride=2), :] = o_ref[:, place * width:(place + 1) * width].T


def finish_kernel(plan, total_rows, in_ref, terms_ref, weight_ref, grad_ref):
    dims = plan.dims
    by_core = [in_ref[pl.ds(core, plan.chips, stride=2), :] for core in range(2)]
    summed = jnp.concatenate([jnp.sum(x.reshape(plan.half, plan.cols, LANES), 1) for x in by_core], 0)
    total = jnp.sum(summed, 0, keepdims=True)
    padded = jnp.concatenate([summed, jnp.zeros((LANES - plan.rows, LANES), jnp.float32)], 0)
    turned = padded.T
    terms = turned[:dims]
    weight = turned[plan.at_weight:plan.at_weight + 1]
    for i in range(1, plan.row_each):
        terms = terms + to_right(turned[i * dims:(i + 1) * dims], i * plan.rows)
        weight = weight + to_right(turned[plan.at_weight + i:plan.at_weight + i + 1], i * plan.rows)
    terms_ref[...] = terms
    weight_ref[...] = weight
    grad_ref[...] = to_left(total, plan.at_grad)[:, :dims] / total_rows


def on_device(x_rows, alpha_rows, x_cols, alpha_cols, lengthscale):
    dims, points = x_rows.shape
    chips = lax.axis_size(CHIPS)
    devices = 2 * chips
    plan = Plan(chips, dims, points)
    whole = pl.BlockSpec(memory_space=pltpu.VMEM)
    f32, bf16 = jnp.float32, jnp.bfloat16

    def exchanged(x, axes):
        blocks = x.reshape(lax.axis_size(axes), 1, -1)
        return lax.all_to_all(blocks, axes, split_axis=0, concat_axis=0, tiled=True).reshape(x.shape)

    sources = (x_rows, alpha_rows.reshape(1, points), x_cols, alpha_cols.reshape(1, points), lengthscale.reshape(1, dims))
    blocks = pl.pallas_call(
        lambda *refs: spread_kernel(plan, *refs),
        out_shape=jax.ShapeDtypeStruct((chips * plan.tiles, LANES), f32),
        in_specs=[pl.BlockSpec(memory_space=pltpu.HBM)] * 5,
        out_specs=whole,
        scratch_shapes=[
            pltpu.VMEM((dims, points), f32),
            pltpu.VMEM((1, points), f32),
            pltpu.VMEM((dims, points), f32),
            pltpu.VMEM((1, points), f32),
            pltpu.VMEM((1, dims), f32),
            pltpu.SemaphoreType.DMA((5,)),
        ],
        compiler_params=pltpu.CompilerParams(vmem_limit_bytes=4 << 20),
        name="spread",
    )(*(pltpu.with_memory_space_constraint(x, pltpu.HBM) for x in sources))
    own = exchanged(blocks, CHIPS)
    other = lax.ppermute(own, CORE, [(0, 1), (1, 0)])
    row_half, col_half = plan.row_each * chips, plan.col_each * chips
    prepared = (
        jax.ShapeDtypeStruct((plan.tiles * LANES, chips), f32),
        jax.ShapeDtypeStruct((col_half, 8 * dims), bf16),
        jax.ShapeDtypeStruct((7 * dims, col_half), bf16),
        jax.ShapeDtypeStruct((8 * dims, row_half), bf16),
    )
    sums = (
        jax.ShapeDtypeStruct((7 * dims, row_half), f32),
        jax.ShapeDtypeStruct((5 * dims, row_half), f32),
    )
    own_parts = pl.pallas_call(
        lambda *refs: own_kernel(plan, *refs),
        out_shape=prepared + sums,
        in_specs=[whole],
        out_specs=(whole,) * 6,
        compiler_params=pltpu.CompilerParams(vmem_limit_bytes=12 << 20),
        cost_estimate=pl.CostEstimate(flops=2 << 30, bytes_accessed=1 << 20, transcendentals=0),
        name="own",
    )(own)
    shares = pl.pallas_call(
        lambda *refs: tile_kernel(plan, *refs),
        out_shape=jax.ShapeDtypeStruct((devices, LANES), f32),
        in_specs=[whole] * 7,
        out_specs=whole,
        scratch_shapes=[
            *(pltpu.VMEM(part.shape, part.dtype) for part in prepared),
            pltpu.VMEM((LANES, devices), f32),
        ],
        compiler_params=pltpu.CompilerParams(vmem_limit_bytes=16 << 20),
        name="tile",
    )(other, *own_parts)
    arrived = exchanged(shares, CHIPS_CORE)
    terms, weight, grad = pl.pallas_call(
        lambda *refs: finish_kernel(plan, points * devices, *refs),
        out_shape=(
            jax.ShapeDtypeStruct((dims, points), f32),
            jax.ShapeDtypeStruct((1, points), f32),
            jax.ShapeDtypeStruct((1, dims), f32),
        ),
        in_specs=[whole],
        out_specs=(whole, whole, whole),
        compiler_params=pltpu.CompilerParams(vmem_limit_bytes=4 << 20),
        name="finish",
    )(arrived)
    return terms, weight.reshape(points), grad.reshape(dims)


def solution(mesh):
    finer = Mesh(mesh.devices.reshape(4, 2, 8, 4), ROW_COL)
    in_specs = (P(None, ROW_COL), P(ROW_COL), P(None, COL_ROW), P(COL_ROW), P())
    out_specs = (P(None, ROW_COL), P(ROW_COL), P())
    return jax.shard_map(on_device, mesh=finer, in_specs=in_specs, out_specs=out_specs, check_vma=False)
```

```python
import math

import jax
import jax.numpy as jnp
from jax import lax
from jax.experimental import pallas as pl
from jax.experimental.pallas import tpu as pltpu
from jax.sharding import Mesh
from jax.sharding import PartitionSpec as P

CORE = "row_1"
CHIPS = ("row_0", "col_0", "col_1")
CHIPS_CORE = (*CHIPS, CORE)
ROW_COL = ("row_0", "row_1", "col_0", "col_1")
COL_ROW = ("col_0", "col_1", "row_0", "row_1")
LOG2E = math.log2(math.e)
LANES = 128
COL_CLASSES = 8
STEP = 1024
ROW_TILE = 256


def split3(x):
    high = x.astype(jnp.bfloat16).astype(jnp.float32)
    rest = x - high
    middle = rest.astype(jnp.bfloat16).astype(jnp.float32)
    return high, middle, rest - middle


def placed_rows(entries, height, lanes):
    row = lax.broadcasted_iota(jnp.int32, (height, lanes), 0)
    block = jnp.zeros((height, lanes), jnp.float32)
    for k, entry in enumerate(entries):
        block = jnp.where(row == k, entry, block)
    return block


def to_left(x, lanes):
    return pltpu.roll(x, (LANES - lanes) % LANES, 1)


def to_right(x, lanes):
    return pltpu.roll(x, lanes % LANES, 1)


class Plan:
    def __init__(self, chips, dims, points):
        self.chips, self.devices, self.dims = chips, 2 * chips, dims
        self.cols = COL_CLASSES
        self.half = chips // self.cols
        self.rows = 2 * self.half
        self.row_each = points // self.rows
        self.col_each = points // self.cols
        self.of_rows = self.row_each * dims
        self.at_cols = 2 * self.of_rows
        self.at_col_alpha = self.at_cols + self.col_each * dims
        self.at_row_alpha = self.at_col_alpha + self.col_each
        self.tiles = pl.cdiv(self.at_row_alpha + 2 * self.row_each, LANES)
        self.at_weight = self.row_each * dims
        self.at_grad = self.at_weight + pl.cdiv(self.row_each, 8) * 8


def spread_kernel(plan, *refs):
    dims = plan.dims
    sources, out_ref, arrived, sems = refs[:5], refs[5], refs[6:11], refs[11]
    loads = [pltpu.make_async_copy(src, dst, sems.at[k]) for k, (src, dst) in enumerate(zip(sources, arrived))]
    for load in loads:
        load.start()
    for load in loads:
        load.wait()
    rows_ref, row_alpha_ref, cols_ref, col_alpha_ref, scale_ref = arrived
    scales = jnp.broadcast_to(scale_ref[:, :dims], (dims, dims))
    down = lax.broadcasted_iota(jnp.int32, (dims, dims), 0)
    along = lax.broadcasted_iota(jnp.int32, (dims, dims), 1)
    inverse = 1.0 / jnp.sum(jnp.where(down == along, scales, 0.0), 1, keepdims=True)
    rows = rows_ref[...] * inverse
    cols = cols_ref[...] * inverse
    of_class = [c * plan.half + i * plan.rows for c in range(2) for i in range(plan.row_each)]
    of_col = [i * plan.cols for i in range(plan.col_each)]
    pieces = [to_left(rows, k) for k in of_class] + [to_left(cols, k) for k in of_col]
    alphas = [to_left(col_alpha_ref[...], k) for k in of_col] + [to_left(row_alpha_ref[...], k) for k in of_class]
    pieces.append(placed_rows(alphas, plan.tiles * LANES - plan.at_col_alpha, LANES))
    stacked = jnp.concatenate(pieces, 0)
    for k in range(plan.tiles):
        turned = stacked[k * LANES:(k + 1) * LANES].T
        lane = lax.broadcasted_iota(jnp.int32, (plan.cols, LANES), 1) + k * LANES
        is_row = (lane < plan.at_cols) | (lane >= plan.at_row_alpha)
        of_cols = turned[:plan.cols]
        for r in range(plan.half):
            of_row = jnp.broadcast_to(turned[r:r + 1], (plan.cols, LANES))
            start = r * plan.cols * plan.tiles + k
            out_ref[pl.ds(start, plan.cols, stride=plan.tiles), :] = jnp.where(is_row, of_row, of_cols)


def prepared_exponents(unit, ones_first):
    dims, width = unit.shape
    scaled = unit * math.sqrt(LOG2E)
    norm = -0.5 * jnp.sum(scaled * scaled, 0, keepdims=True)
    parts = split3(norm)
    ones = (1.0, 1.0, 1.0)
    norms = placed_rows(ones + parts if ones_first else parts + ones, dims, width)
    h, m, l = split3(scaled)
    if ones_first:
        return h, m, h, m, l, h, norms
    return h, h, m, m, h, l, norms


def prepare_rows(plan, in_ref, t_ref, a_ref):
    dims, width = plan.dims, plan.chips
    bf16 = jnp.bfloat16
    core = lax.axis_index(CORE)
    for k in range(plan.tiles):
        t_ref[k * LANES:(k + 1) * LANES, :] = in_ref[pl.ds(k, width, stride=plan.tiles), :].T
    for i in range(plan.row_each):
        unit = t_ref[pl.ds(pl.multiple_of(core * plan.of_rows, 8) + i * dims, dims), :]
        for g, block in enumerate(prepared_exponents(unit, False)):
            a_ref[g * dims:(g + 1) * dims, i * width:(i + 1) * width] = block.astype(bf16)


def prepare_cols(plan, t_ref, b_ref, v_ref):
    dims, width = plan.dims, plan.chips
    bf16 = jnp.bfloat16
    for i in range(plan.col_each):
        at = plan.at_cols + i * dims
        unit = t_ref[at:at + dims, :]
        alpha = t_ref[plan.at_col_alpha + i:plan.at_col_alpha + i + 1, :]
        b_ref[i * width:(i + 1) * width, :] = jnp.concatenate(prepared_exponents(unit, True), 0).astype(bf16).T
        weighted = alpha * unit
        fh, fm, fl = split3(weighted)
        sh, sm, sl = split3(weighted * unit)
        alphas = placed_rows(split3(alpha), dims, width)
        for g, block in enumerate((fh, fm, sh, sm, alphas, fl, sl)):
            v_ref[g * dims:(g + 1) * dims, i * width:(i + 1) * width] = block.astype(bf16)


def add_columns(plan, sums, a_tiles, b_ref, v_ref, step):
    f32, bf16 = jnp.float32, jnp.bfloat16
    sums = list(sums)
    for start in range(0, b_ref.shape[0], step):
        points = b_ref[start:start + step, :]
        values = v_ref[:, start:start + step]
        kernels = [jnp.exp2(jnp.dot(points, a_tile, preferred_element_type=f32)) for a_tile in a_tiles]
        highs = [kernel.astype(bf16) for kernel in kernels]
        lows = [(kernel - high.astype(f32)).astype(bf16) for kernel, high in zip(kernels, highs)]
        bigs = [jnp.dot(values, high, preferred_element_type=f32) for high in highs]
        smalls = [jnp.dot(values[:5 * plan.dims], low, preferred_element_type=f32) for low in lows]
        sums = [(s[0] + big, s[1] + small) for s, big, small in zip(sums, bigs, smalls)]
    return sums


def zero_sums(plan):
    return jnp.zeros((7 * plan.dims, ROW_TILE), jnp.float32), jnp.zeros((5 * plan.dims, ROW_TILE), jnp.float32)


def own_kernel(plan, own_ref, t_ref, b_ref, v_ref, a_ref, big_ref, small_ref):
    prepare_rows(plan, own_ref, t_ref, a_ref)
    prepare_cols(plan, t_ref, b_ref, v_ref)
    cuts = row_cuts(a_ref)
    for cut in cuts:
        (big, small), = add_columns(plan, [zero_sums(plan)], [a_ref[:, cut]], b_ref, v_ref, STEP)
        big_ref[:, cut], small_ref[:, cut] = big, small


def row_cuts(a_ref):
    return [slice(start, start + ROW_TILE) for start in range(0, a_ref.shape[1], ROW_TILE)]


def tile_kernel(plan, other_ref, own_t_ref, own_b_ref, own_v_ref, own_a_ref, big_ref, small_ref, out_ref, t_ref, b_ref, v_ref, a_ref, o_ref):
    dims, width = plan.dims, plan.chips
    prepare_rows(plan, other_ref, t_ref, a_ref)
    cuts = row_cuts(a_ref)
    other_sums = add_columns(plan, [zero_sums(plan)] * len(cuts), [a_ref[:, cut] for cut in cuts], own_b_ref, own_v_ref, STEP)
    prepare_cols(plan, t_ref, b_ref, v_ref)
    core = lax.axis_index(CORE)
    grad = jnp.zeros((dims, width), jnp.float32)
    o_ref[plan.at_weight:, :] = jnp.zeros((LANES - plan.at_weight, 2 * width), jnp.float32)
    tiles = [(own_t_ref, own_a_ref, cut, core) for cut in cuts] + [(t_ref, a_ref, cut, 1 - core) for cut in cuts]
    sums = [(big_ref[:, cut], small_ref[:, cut]) for cut in cuts] + other_sums
    sums = add_columns(plan, sums, [rows_ref[:, cut] for _, rows_ref, cut, _ in tiles], b_ref, v_ref, STEP)
    for (points_ref, _, cut, place), (big, small) in zip(tiles, sums):
        lanes = pl.ds(pl.multiple_of(place * width, LANES), width)
        start = cut.start

        def part(x, g):
            return x[g * dims:(g + 1) * dims]

        first = (part(small, 0) + part(small, 1) + part(big, 5)) + part(big, 1) + part(big, 0)
        second = (part(small, 2) + part(small, 3) + part(big, 6)) + part(big, 3) + part(big, 2)
        weights = part(big, 4) + part(small, 4)
        weight = weights[0:1] + weights[1:2] + weights[2:3]
        for i in range(start // width, (start + ROW_TILE) // width):
            cut = slice(i * width - start, (i + 1) * width - start)
            unit = points_ref[pl.ds(pl.multiple_of(core * plan.of_rows, 8) + i * dims, dims), :]
            alpha = points_ref[pl.ds(plan.at_row_alpha + core * plan.row_each + i, 1), :]
            terms = 0.5 * alpha * (unit * unit * weight[:, cut] - 2.0 * unit * first[:, cut] + second[:, cut])
            o_ref[i * dims:(i + 1) * dims, lanes] = terms
            o_ref[plan.at_weight + i:plan.at_weight + i + 1, lanes] = weight[:, cut]
            grad = grad + terms
    share = jnp.sum(grad, 1, keepdims=True)
    o_ref[plan.at_grad:plan.at_grad + dims, :] = jnp.broadcast_to(share, (dims, 2 * width))
    for place in range(2):
        out_ref[pl.ds(place, width, stride=2), :] = o_ref[:, place * width:(place + 1) * width].T


def finish_kernel(plan, total_rows, in_ref, terms_ref, weight_ref, grad_ref):
    dims = plan.dims
    by_core = [in_ref[pl.ds(core, plan.chips, stride=2), :] for core in range(2)]
    summed = jnp.concatenate([jnp.sum(x.reshape(plan.half, plan.cols, LANES), 1) for x in by_core], 0)
    total = jnp.sum(summed, 0, keepdims=True)
    padded = jnp.concatenate([summed, jnp.zeros((LANES - plan.rows, LANES), jnp.float32)], 0)
    turned = padded.T
    terms = turned[:dims]
    weight = turned[plan.at_weight:plan.at_weight + 1]
    for i in range(1, plan.row_each):
        terms = terms + to_right(turned[i * dims:(i + 1) * dims], i * plan.rows)
        weight = weight + to_right(turned[plan.at_weight + i:plan.at_weight + i + 1], i * plan.rows)
    terms_ref[...] = terms
    weight_ref[...] = weight
    grad_ref[...] = to_left(total, plan.at_grad)[:, :dims] / total_rows


def on_device(x_rows, alpha_rows, x_cols, alpha_cols, lengthscale):
    dims, points = x_rows.shape
    chips = lax.axis_size(CHIPS)
    devices = 2 * chips
    plan = Plan(chips, dims, points)
    whole = pl.BlockSpec(memory_space=pltpu.VMEM)
    f32, bf16 = jnp.float32, jnp.bfloat16

    def exchanged(x, axes):
        blocks = x.reshape(lax.axis_size(axes), 1, -1)
        return lax.all_to_all(blocks, axes, split_axis=0, concat_axis=0, tiled=True).reshape(x.shape)

    sources = (x_rows, alpha_rows.reshape(1, points), x_cols, alpha_cols.reshape(1, points), lengthscale.reshape(1, dims))
    blocks = pl.pallas_call(
        lambda *refs: spread_kernel(plan, *refs),
        out_shape=jax.ShapeDtypeStruct((chips * plan.tiles, LANES), f32),
        in_specs=[pl.BlockSpec(memory_space=pltpu.HBM)] * 5,
        out_specs=whole,
        scratch_shapes=[
            pltpu.VMEM((dims, points), f32),
            pltpu.VMEM((1, points), f32),
            pltpu.VMEM((dims, points), f32),
            pltpu.VMEM((1, points), f32),
            pltpu.VMEM((1, dims), f32),
            pltpu.SemaphoreType.DMA((5,)),
        ],
        compiler_params=pltpu.CompilerParams(vmem_limit_bytes=4 << 20),
        name="spread",
    )(*(pltpu.with_memory_space_constraint(x, pltpu.HBM) for x in sources))
    own = exchanged(blocks, CHIPS)
    other = lax.ppermute(own, CORE, [(0, 1), (1, 0)])
    row_half, col_half = plan.row_each * chips, plan.col_each * chips
    prepared = (
        jax.ShapeDtypeStruct((plan.tiles * LANES, chips), f32),
        jax.ShapeDtypeStruct((col_half, 7 * dims), bf16),
        jax.ShapeDtypeStruct((7 * dims, col_half), bf16),
        jax.ShapeDtypeStruct((7 * dims, row_half), bf16),
    )
    sums = (
        jax.ShapeDtypeStruct((7 * dims, row_half), f32),
        jax.ShapeDtypeStruct((5 * dims, row_half), f32),
    )
    own_parts = pl.pallas_call(
        lambda *refs: own_kernel(plan, *refs),
        out_shape=prepared + sums,
        in_specs=[whole],
        out_specs=(whole,) * 6,
        compiler_params=pltpu.CompilerParams(vmem_limit_bytes=12 << 20),
        cost_estimate=pl.CostEstimate(flops=2 << 30, bytes_accessed=1 << 20, transcendentals=0),
        name="own",
    )(own)
    shares = pl.pallas_call(
        lambda *refs: tile_kernel(plan, *refs),
        out_shape=jax.ShapeDtypeStruct((devices, LANES), f32),
        in_specs=[whole] * 7,
        out_specs=whole,
        scratch_shapes=[
            *(pltpu.VMEM(part.shape, part.dtype) for part in prepared),
            pltpu.VMEM((LANES, devices), f32),
        ],
        compiler_params=pltpu.CompilerParams(vmem_limit_bytes=16 << 20),
        name="tile",
    )(other, *own_parts)
    arrived = exchanged(shares, CHIPS_CORE)
    terms, weight, grad = pl.pallas_call(
        lambda *refs: finish_kernel(plan, points * devices, *refs),
        out_shape=(
            jax.ShapeDtypeStruct((dims, points), f32),
            jax.ShapeDtypeStruct((1, points), f32),
            jax.ShapeDtypeStruct((1, dims), f32),
        ),
        in_specs=[whole],
        out_specs=(whole, whole, whole),
        compiler_params=pltpu.CompilerParams(vmem_limit_bytes=4 << 20),
        name="finish",
    )(arrived)
    return terms, weight.reshape(points), grad.reshape(dims)


def solution(mesh):
    finer = Mesh(mesh.devices.reshape(4, 2, 8, 4), ROW_COL)
    in_specs = (P(None, ROW_COL), P(ROW_COL), P(None, COL_ROW), P(COL_ROW), P())
    out_specs = (P(None, ROW_COL), P(ROW_COL), P())
    return jax.shard_map(on_device, mesh=finer, in_specs=in_specs, out_specs=out_specs, check_vma=False)
```

```python
import math

import jax
import jax.numpy as jnp
from jax import lax
from jax.experimental import pallas as pl
from jax.experimental.pallas import tpu as pltpu
from jax.sharding import Mesh
from jax.sharding import PartitionSpec as P

CORE = "row_1"
CHIPS = ("col_1", "col_0", "row_0")
CHIPS_CORE = (*CHIPS, CORE)
ROW_COL = ("row_0", "row_1", "col_0", "col_1")
COL_ROW = ("col_0", "col_1", "row_0", "row_1")
LOG2E = math.log2(math.e)
LANES = 128
COL_CLASSES = 8
STEP = 1024
ROW_TILE = 256


def split3(x):
    high = x.astype(jnp.bfloat16).astype(jnp.float32)
    rest = x - high
    middle = rest.astype(jnp.bfloat16).astype(jnp.float32)
    return high, middle, rest - middle


def placed_rows(entries, height, lanes):
    row = lax.broadcasted_iota(jnp.int32, (height, lanes), 0)
    block = jnp.zeros((height, lanes), jnp.float32)
    for k, entry in enumerate(entries):
        block = jnp.where(row == k, entry, block)
    return block


def to_left(x, lanes):
    return pltpu.roll(x, (LANES - lanes) % LANES, 1)


def to_right(x, lanes):
    return pltpu.roll(x, lanes % LANES, 1)


class Plan:
    def __init__(self, chips, dims, points):
        self.chips, self.devices, self.dims = chips, 2 * chips, dims
        self.cols = COL_CLASSES
        self.half = chips // self.cols
        self.rows = 2 * self.half
        self.row_each = points // self.rows
        self.col_each = points // self.cols
        self.of_rows = self.row_each * dims
        self.at_cols = 2 * self.of_rows
        self.at_col_alpha = self.at_cols + self.col_each * dims
        self.at_row_alpha = self.at_col_alpha + self.col_each
        self.tiles = pl.cdiv(self.at_row_alpha + 2 * self.row_each, LANES)
        self.at_weight = self.row_each * dims
        self.at_grad = self.at_weight + pl.cdiv(self.row_each, 8) * 8


def spread_kernel(plan, *refs):
    dims = plan.dims
    sources, out_ref, arrived, sems = refs[:5], refs[5], refs[6:11], refs[11]
    loads = [pltpu.make_async_copy(src, dst, sems.at[k]) for k, (src, dst) in enumerate(zip(sources, arrived))]
    for load in loads:
        load.start()
    for load in loads:
        load.wait()
    rows_ref, row_alpha_ref, cols_ref, col_alpha_ref, scale_ref = arrived
    scales = jnp.broadcast_to(scale_ref[:, :dims], (dims, dims))
    down = lax.broadcasted_iota(jnp.int32, (dims, dims), 0)
    along = lax.broadcasted_iota(jnp.int32, (dims, dims), 1)
    inverse = 1.0 / jnp.sum(jnp.where(down == along, scales, 0.0), 1, keepdims=True)
    rows = rows_ref[...] * inverse
    cols = cols_ref[...] * inverse
    of_class = [c * plan.half + i * plan.rows for c in range(2) for i in range(plan.row_each)]
    of_col = [i * plan.cols for i in range(plan.col_each)]
    pieces = [to_left(rows, k) for k in of_class] + [to_left(cols, k) for k in of_col]
    alphas = [to_left(col_alpha_ref[...], k) for k in of_col] + [to_left(row_alpha_ref[...], k) for k in of_class]
    pieces.append(placed_rows(alphas, plan.tiles * LANES - plan.at_col_alpha, LANES))
    stacked = jnp.concatenate(pieces, 0)
    for k in range(plan.tiles):
        turned = stacked[k * LANES:(k + 1) * LANES].T
        lane = lax.broadcasted_iota(jnp.int32, (plan.cols, LANES), 1) + k * LANES
        is_row = (lane < plan.at_cols) | (lane >= plan.at_row_alpha)
        of_cols = turned[:plan.cols]
        for r in range(plan.half):
            of_row = jnp.broadcast_to(turned[r:r + 1], (plan.cols, LANES))
            start = r * plan.cols * plan.tiles + k
            out_ref[pl.ds(start, plan.cols, stride=plan.tiles), :] = jnp.where(is_row, of_row, of_cols)


def prepared_exponents(unit, ones_first):
    dims, width = unit.shape
    scaled = unit * math.sqrt(LOG2E)
    norm = -0.5 * jnp.sum(scaled * scaled, 0, keepdims=True)
    parts = split3(norm)
    ones = (1.0, 1.0, 1.0)
    norms = placed_rows(ones + parts if ones_first else parts + ones, dims, width)
    h, m, l = split3(scaled)
    if ones_first:
        return h, m, h, m, l, h, norms, jnp.zeros_like(norms)
    return h, h, m, m, h, l, norms, jnp.zeros_like(norms)


def prepare_rows(plan, in_ref, t_ref, a_ref):
    dims, width = plan.dims, plan.chips
    bf16 = jnp.bfloat16
    core = lax.axis_index(CORE)
    for k in range(plan.tiles):
        t_ref[k * LANES:(k + 1) * LANES, :] = in_ref[pl.ds(k, width, stride=plan.tiles), :].T
    for i in range(plan.row_each):
        unit = t_ref[pl.ds(pl.multiple_of(core * plan.of_rows, 8) + i * dims, dims), :]
        for g, block in enumerate(prepared_exponents(unit, False)):
            a_ref[g * dims:(g + 1) * dims, i * width:(i + 1) * width] = block.astype(bf16)


def prepare_cols(plan, t_ref, b_ref, v_ref):
    dims, width = plan.dims, plan.chips
    bf16 = jnp.bfloat16
    for i in range(plan.col_each):
        at = plan.at_cols + i * dims
        unit = t_ref[at:at + dims, :]
        alpha = t_ref[plan.at_col_alpha + i:plan.at_col_alpha + i + 1, :]
        b_ref[i * width:(i + 1) * width, :] = jnp.concatenate(prepared_exponents(unit, True), 0).astype(bf16).T
        weighted = alpha * unit
        fh, fm, fl = split3(weighted)
        sh, sm, sl = split3(weighted * unit)
        alphas = placed_rows(split3(alpha), dims, width)
        for g, block in enumerate((fh, fm, sh, sm, alphas, fl, sl)):
            v_ref[g * dims:(g + 1) * dims, i * width:(i + 1) * width] = block.astype(bf16)


def add_columns(plan, sums, a_tiles, b_ref, v_ref, step):
    f32, bf16 = jnp.float32, jnp.bfloat16
    sums = list(sums)
    for start in range(0, b_ref.shape[0], step):
        points = b_ref[start:start + step, :]
        values = v_ref[:, start:start + step]
        kernels = [jnp.exp2(jnp.dot(points, a_tile, preferred_element_type=f32)) for a_tile in a_tiles]
        highs = [kernel.astype(bf16) for kernel in kernels]
        lows = [(kernel - high.astype(f32)).astype(bf16) for kernel, high in zip(kernels, highs)]
        bigs = [jnp.dot(values, high, preferred_element_type=f32) for high in highs]
        smalls = [jnp.dot(values[:5 * plan.dims], low, preferred_element_type=f32) for low in lows]
        sums = [(s[0] + big, s[1] + small) for s, big, small in zip(sums, bigs, smalls)]
    return sums


def zero_sums(plan):
    return jnp.zeros((7 * plan.dims, ROW_TILE), jnp.float32), jnp.zeros((5 * plan.dims, ROW_TILE), jnp.float32)


def own_kernel(plan, own_ref, t_ref, b_ref, v_ref, a_ref, big_ref, small_ref):
    prepare_rows(plan, own_ref, t_ref, a_ref)
    prepare_cols(plan, t_ref, b_ref, v_ref)
    cuts = row_cuts(a_ref)
    for cut in cuts:
        (big, small), = add_columns(plan, [zero_sums(plan)], [a_ref[:, cut]], b_ref, v_ref, STEP)
        big_ref[:, cut], small_ref[:, cut] = big, small


def row_cuts(a_ref):
    return [slice(start, start + ROW_TILE) for start in range(0, a_ref.shape[1], ROW_TILE)]


def tile_kernel(plan, other_ref, own_t_ref, own_b_ref, own_v_ref, own_a_ref, big_ref, small_ref, out_ref, t_ref, b_ref, v_ref, a_ref, o_ref):
    dims, width = plan.dims, plan.chips
    prepare_rows(plan, other_ref, t_ref, a_ref)
    cuts = row_cuts(a_ref)
    other_sums = add_columns(plan, [zero_sums(plan)] * len(cuts), [a_ref[:, cut] for cut in cuts], own_b_ref, own_v_ref, STEP)
    prepare_cols(plan, t_ref, b_ref, v_ref)
    core = lax.axis_index(CORE)
    grad = jnp.zeros((dims, width), jnp.float32)
    o_ref[plan.at_weight:, :] = jnp.zeros((LANES - plan.at_weight, 2 * width), jnp.float32)
    tiles = [(own_t_ref, own_a_ref, cut, core) for cut in cuts] + [(t_ref, a_ref, cut, 1 - core) for cut in cuts]
    sums = [(big_ref[:, cut], small_ref[:, cut]) for cut in cuts] + other_sums
    sums = add_columns(plan, sums, [rows_ref[:, cut] for _, rows_ref, cut, _ in tiles], b_ref, v_ref, STEP)
    for (points_ref, _, cut, place), (big, small) in zip(tiles, sums):
        lanes = pl.ds(pl.multiple_of(place * width, LANES), width)
        start = cut.start

        def part(x, g):
            return x[g * dims:(g + 1) * dims]

        first = (part(small, 0) + part(small, 1) + part(big, 5)) + part(big, 1) + part(big, 0)
        second = (part(small, 2) + part(small, 3) + part(big, 6)) + part(big, 3) + part(big, 2)
        weights = part(big, 4) + part(small, 4)
        weight = weights[0:1] + weights[1:2] + weights[2:3]
        for i in range(start // width, (start + ROW_TILE) // width):
            cut = slice(i * width - start, (i + 1) * width - start)
            unit = points_ref[pl.ds(pl.multiple_of(core * plan.of_rows, 8) + i * dims, dims), :]
            alpha = points_ref[pl.ds(plan.at_row_alpha + core * plan.row_each + i, 1), :]
            terms = 0.5 * alpha * (unit * unit * weight[:, cut] - 2.0 * unit * first[:, cut] + second[:, cut])
            o_ref[i * dims:(i + 1) * dims, lanes] = terms
            o_ref[plan.at_weight + i:plan.at_weight + i + 1, lanes] = weight[:, cut]
            grad = grad + terms
    share = jnp.sum(grad, 1, keepdims=True)
    o_ref[plan.at_grad:plan.at_grad + dims, :] = jnp.broadcast_to(share, (dims, 2 * width))
    for place in range(2):
        out_ref[pl.ds(place, width, stride=2), :] = o_ref[:, place * width:(place + 1) * width].T


def finish_kernel(plan, total_rows, in_ref, terms_ref, weight_ref, grad_ref):
    dims = plan.dims
    by_core = [in_ref[pl.ds(core, plan.chips, stride=2), :] for core in range(2)]
    summed = jnp.concatenate([jnp.sum(x.reshape(plan.half, plan.cols, LANES), 1) for x in by_core], 0)
    total = jnp.sum(summed, 0, keepdims=True)
    padded = jnp.concatenate([summed, jnp.zeros((LANES - plan.rows, LANES), jnp.float32)], 0)
    turned = padded.T
    terms = turned[:dims]
    weight = turned[plan.at_weight:plan.at_weight + 1]
    for i in range(1, plan.row_each):
        terms = terms + to_right(turned[i * dims:(i + 1) * dims], i * plan.rows)
        weight = weight + to_right(turned[plan.at_weight + i:plan.at_weight + i + 1], i * plan.rows)
    terms_ref[...] = terms
    weight_ref[...] = weight
    grad_ref[...] = to_left(total, plan.at_grad)[:, :dims] / total_rows


def on_device(x_rows, alpha_rows, x_cols, alpha_cols, lengthscale):
    dims, points = x_rows.shape
    chips = lax.axis_size(CHIPS)
    devices = 2 * chips
    plan = Plan(chips, dims, points)
    whole = pl.BlockSpec(memory_space=pltpu.VMEM)
    f32, bf16 = jnp.float32, jnp.bfloat16

    def exchanged(x, axes):
        blocks = x.reshape(lax.axis_size(axes), 1, -1)
        return lax.all_to_all(blocks, axes, split_axis=0, concat_axis=0, tiled=True).reshape(x.shape)

    sources = (x_rows, alpha_rows.reshape(1, points), x_cols, alpha_cols.reshape(1, points), lengthscale.reshape(1, dims))
    blocks = pl.pallas_call(
        lambda *refs: spread_kernel(plan, *refs),
        out_shape=jax.ShapeDtypeStruct((chips * plan.tiles, LANES), f32),
        in_specs=[pl.BlockSpec(memory_space=pltpu.HBM)] * 5,
        out_specs=whole,
        scratch_shapes=[
            pltpu.VMEM((dims, points), f32),
            pltpu.VMEM((1, points), f32),
            pltpu.VMEM((dims, points), f32),
            pltpu.VMEM((1, points), f32),
            pltpu.VMEM((1, dims), f32),
            pltpu.SemaphoreType.DMA((5,)),
        ],
        compiler_params=pltpu.CompilerParams(vmem_limit_bytes=4 << 20),
        name="spread",
    )(*(pltpu.with_memory_space_constraint(x, pltpu.HBM) for x in sources))
    own = exchanged(blocks, CHIPS)
    other = lax.ppermute(own, CORE, [(0, 1), (1, 0)])
    row_half, col_half = plan.row_each * chips, plan.col_each * chips
    prepared = (
        jax.ShapeDtypeStruct((plan.tiles * LANES, chips), f32),
        jax.ShapeDtypeStruct((col_half, 8 * dims), bf16),
        jax.ShapeDtypeStruct((7 * dims, col_half), bf16),
        jax.ShapeDtypeStruct((8 * dims, row_half), bf16),
    )
    sums = (
        jax.ShapeDtypeStruct((7 * dims, row_half), f32),
        jax.ShapeDtypeStruct((5 * dims, row_half), f32),
    )
    own_parts = pl.pallas_call(
        lambda *refs: own_kernel(plan, *refs),
        out_shape=prepared + sums,
        in_specs=[whole],
        out_specs=(whole,) * 6,
        compiler_params=pltpu.CompilerParams(vmem_limit_bytes=12 << 20),
        cost_estimate=pl.CostEstimate(flops=2 << 30, bytes_accessed=1 << 20, transcendentals=0),
        name="own",
    )(own)
    shares = pl.pallas_call(
        lambda *refs: tile_kernel(plan, *refs),
        out_shape=jax.ShapeDtypeStruct((devices, LANES), f32),
        in_specs=[whole] * 7,
        out_specs=whole,
        scratch_shapes=[
            *(pltpu.VMEM(part.shape, part.dtype) for part in prepared),
            pltpu.VMEM((LANES, devices), f32),
        ],
        compiler_params=pltpu.CompilerParams(vmem_limit_bytes=16 << 20),
        name="tile",
    )(other, *own_parts)
    arrived = exchanged(shares, CHIPS_CORE)
    terms, weight, grad = pl.pallas_call(
        lambda *refs: finish_kernel(plan, points * devices, *refs),
        out_shape=(
            jax.ShapeDtypeStruct((dims, points), f32),
            jax.ShapeDtypeStruct((1, points), f32),
            jax.ShapeDtypeStruct((1, dims), f32),
        ),
        in_specs=[whole],
        out_specs=(whole, whole, whole),
        compiler_params=pltpu.CompilerParams(vmem_limit_bytes=4 << 20),
        name="finish",
    )(arrived)
    return terms, weight.reshape(points), grad.reshape(dims)


def solution(mesh):
    finer = Mesh(mesh.devices.reshape(4, 2, 8, 4), ROW_COL)
    in_specs = (P(None, ROW_COL), P(ROW_COL), P(None, COL_ROW), P(COL_ROW), P())
    out_specs = (P(None, ROW_COL), P(ROW_COL), P())
    return jax.shard_map(on_device, mesh=finer, in_specs=in_specs, out_specs=out_specs, check_vma=False)
```
